32 devices in a mesh: cohort: 2 (over y), bx: 16 (over z, x, core).
Axes of the slice: x: 2, y: 2, z: 4, core: 2. Of those that a mesh axis runs over, the one named last changes fastest.
Arguments:
- bold: bfloat16 [256, 12, 4096], P('cohort', None, 'bx'), parts along dimension 0, may hold values from -6 to 6
- nbr_table: int32 [256, 4096], P('cohort', 'bx'), parts along dimension 0, may hold values from -1 to 767, as said below
- subject: int32 [256], P('cohort'), parts along dimension 0, may hold values from 0 to 7
Outputs:
- spread: float32 [8192], P(('cohort', 'bx')), parts along dimension 0
- gram_mean: float32 [256, 128], P('cohort'), parts along dimension 0
The draws below stay inside these ranges and needn't reach their ends.
There are 2 independent parts, one for each index of `cohort`. The reference program is written for one: setup_inputs(seed, part) draws one part's arguments, and reference() takes and returns one part's arrays. A program takes and returns all parts, laid end to end along the dimension named above; each array names one. Nothing has to cross between parts.
Inputs may be any that keep to these rules, and one draw needn't show every extreme that they name: `nbr_table`: rows 125 to 127 are all -1 and row (124) // 2 names the centre itself (256 + its place in its block). Any other entry is -1 or the place, in the window made of the previous block, the centre's own block and the next block (768 voxels in order), of a voxel at most 147 voxels away from the centre in voxel order; no entry names a voxel outside the cohort's 4096 voxels.
All inputs are finite; a program needn't handle non-finite values.
Results may differ from the reference program's by a relative error of at most 0.0003.
Values may be sent and summed in bfloat16 or wider, within the bound.
A program may use at most 64 MiB of HBM per device.

```python
import jax
import jax.numpy as jnp
from jax import lax

VB = 256
E = 128
TP = 12
NB = 125
NBP = 128
SUBJ = 8
ROW = 8
PLANE = 64
NVOX = 4096
N_BX = 16


def draw_nbr_table(key, part):
    member = jnp.arange(NB, dtype=jnp.int32)
    along_x = member // 25 - 2
    along_y = member // 5 % 5 - 2
    along_z = member % 5 - 2
    base_offset = along_x * PLANE + along_y * ROW + along_z
    is_centre = (member == (NB - 1) // 2)[:, None]
    subkeys = jax.random.split(key, 2)
    jitter = jax.random.randint(subkeys[0], (NB, NVOX), -1, 2).astype(jnp.int32)
    jitter = jnp.where(is_centre, 0, jitter)
    keeping = jax.random.randint(subkeys[1], (NB, NVOX), 0, 4) > 0
    keeping = keeping | is_centre
    centre_ids = jnp.arange(NVOX, dtype=jnp.int32)[None, :]
    target = centre_ids + base_offset[:, None] + jitter
    inside = keeping & (target >= 0) & (target < NVOX)
    local_place = target - (centre_ids // VB - 1) * VB
    table = jnp.where(inside, local_place, -1).astype(jnp.int32)
    padding = jnp.full((NBP - NB, NVOX), -1, jnp.int32)
    return jnp.concatenate([table, padding], axis=0)


def plant(array, rng, least, top_value):
    shape = array.shape
    index_at = [jax.random.randint(jax.random.fold_in(rng, axis), (), 0, shape[axis]) for axis in range(len(shape))]
    array = array.at[tuple(index_at)].set(least)
    longest = shape.index(max(shape))
    index_at[longest] = (index_at[longest] + 1) % shape[longest]
    return array.at[tuple(index_at)].set(top_value)


def levels(rng, extent, cuts, low, top_value):
    gain = 1.0
    for dim, shards_of in cuts:
        heights = jax.random.uniform(jax.random.fold_in(jax.random.fold_in(rng, 6), dim), (shards_of,), jnp.float32, low / len(cuts), top_value / len(cuts))
        gain = gain * jnp.repeat(jnp.exp(heights), extent[dim] // shards_of).reshape((-1,) + (1,) * (len(extent) - 1 - dim))
    return gain


def normal_values(rng, dims, scale, limit, shards=(), held_as=jnp.bfloat16):
    values = jax.random.normal(rng, dims, jnp.float32) * scale
    if len(shards) > 0:
        values = levels(rng, dims, shards, -0.22, 0.18) * values
    return jnp.clip(values, min=-limit, max=limit).astype(held_as)


def setup_inputs(seed: int = 0, part: int = 0) -> dict:
    key_list = jax.random.split(jax.random.key(seed), 4)
    part_keys = jax.random.split(jax.random.fold_in(key_list[3], part), 4)
    bold = normal_values(part_keys[0], (E, TP, NVOX), 1.0, 6.0, ((2, 16),))
    nbr_table = draw_nbr_table(jax.random.fold_in(jax.random.fold_in(key_list[3], part), 71), part)
    subject = plant(jax.random.randint(part_keys[2], (E,), 0, SUBJ), jax.random.fold_in(part_keys[2], 1), 0, SUBJ - 1).astype(jnp.int32)
    return dict(bold=bold, nbr_table=nbr_table, subject=subject)


VARIANCE_FLOOR = 0.05

def normalize(series):
    values = series.astype(jnp.float32)
    centred = values - lax.optimization_barrier(jnp.mean(values, axis=1, keepdims=True))
    divisor = jnp.sqrt(lax.optimization_barrier(jnp.sum(centred * centred, axis=1, keepdims=True)) + 1.0)
    return (centred / divisor).astype(jnp.bfloat16)

def zscore(correl, onehot, counts):
    averages = jnp.einsum('es,ecj->scj', onehot, correl, precision=lax.Precision.HIGHEST) / counts[:, None, None]
    expanded = jnp.einsum('es,scj->ecj', onehot, averages, precision=lax.Precision.HIGHEST)
    deviation = correl - expanded
    variance = jnp.einsum('es,ecj->scj', onehot, deviation * deviation, precision=lax.Precision.HIGHEST) / counts[:, None, None]
    divisor = jnp.einsum('es,scj->ecj', onehot, jnp.sqrt(variance + VARIANCE_FLOOR), precision=lax.Precision.HIGHEST)
    return deviation / divisor

def reference(bold, nbr_table, subject):
    normed = normalize(bold).astype(jnp.float32)
    onehot = (subject[:, None] == jnp.arange(SUBJ, dtype=jnp.int32)[None, :]).astype(jnp.float32)
    counts = jnp.maximum(lax.optimization_barrier(jnp.sum(onehot, axis=0)), 1.0)
    padded = jnp.pad(normed, ((0, 0), (0, 0), (VB, VB)))

    def one_block(block_id):
        first_col = (block_id * VB).astype(jnp.int32)
        lookup = lax.dynamic_slice_in_dim(nbr_table, first_col, VB, 1)
        usable = (lookup >= 0).T
        position = (jnp.where(lookup >= 0, lookup, 0) + first_col).T.reshape(-1).astype(jnp.int32)
        centre = lax.dynamic_slice_in_dim(normed, first_col, VB, 2)
        gathered = jnp.take(padded, position, axis=2).reshape(E, TP, VB, NBP)
        correl = jnp.einsum('etc,etcj->ecj', centre, gathered, precision=lax.Precision.HIGHEST)
        correl = jnp.where(usable[None], correl, jnp.float32(0.0))
        features = zscore(correl, onehot, counts)
        kernel = jnp.einsum('ecj,fcj->cef', features, features, precision=lax.Precision.HIGHEST) / NB
        return (lax.optimization_barrier(jnp.sum(kernel, axis=0)), jnp.sqrt(lax.optimization_barrier(jnp.sum(kernel * kernel, axis=(1, 2))) / E))
    block_sums, spreads = lax.map(one_block, jnp.arange(N_BX).astype(jnp.int32))
    return (spreads.reshape(-1), lax.optimization_barrier(jnp.sum(block_sums, axis=0)) / NVOX)
```

```python
import functools

import jax
import jax.numpy as jnp
from jax import lax
from jax.experimental import pallas as pl
from jax.experimental.pallas import tpu as pltpu
from jax.sharding import PartitionSpec as P

NB = 125
SUBJ = 8
REACH = 147
VARIANCE_FLOOR = 0.05

LANES = 128
ROWS = 8
GROUP = 8
CHUNK = 64
LEAD = 160
SPAN = 384
MESH = pl.DeviceIdType.MESH
BY_ROW = lax.GatherDimensionNumbers(
    offset_dims=(), collapsed_slice_dims=(0,), start_index_map=(0,),
    operand_batching_dims=(1,), start_indices_batching_dims=(1,))
BY_LANE = lax.GatherDimensionNumbers(
    offset_dims=(), collapsed_slice_dims=(1,), start_index_map=(1,),
    operand_batching_dims=(0,), start_indices_batching_dims=(0,))


def take(values, at, dims):
    return lax.gather(values, at[..., None], dims, (1, 1), mode="promise_in_bounds")


def normalized(values):
    points = values.shape[0]
    centred = values - jnp.sum(values, axis=0, keepdims=True) * (1.0 / points)
    return centred * (1.0 / jnp.sqrt(jnp.sum(centred * centred, axis=0, keepdims=True) + 1.0))


def features_kernel(ext_ref, idx_ref, subject_ref, spread_ref, gram_ref,
                    sorted_ref, win_ref, own_ref, lane_ref, tile_ref, valid_ref, sid_ref, perm_ref,
                    x0_ref, x1_ref, sum0_ref, sum1_ref, sq0_ref, sq1_ref, mean0_ref, mean1_ref,
                    scale0_ref, scale1_ref, square_ref, total_ref):
    points, epochs, wide = ext_ref.shape
    slots, block_len = idx_ref.shape
    groups = epochs // GROUP
    depth = points * GROUP
    span = SPAN + LANES

    named = jnp.broadcast_to(subject_ref[...], (epochs, LANES))
    named_t = named.T
    row = lax.broadcasted_iota(jnp.int32, (epochs, LANES), 0)
    col = lax.broadcasted_iota(jnp.int32, (epochs, LANES), 1)
    ahead = (named_t < named) | ((named_t == named) & (row < col))
    rank = jnp.sum(ahead.astype(jnp.float32), axis=0, keepdims=True).astype(jnp.int32)
    perm = (jnp.broadcast_to(rank, (epochs, LANES)) == row).astype(jnp.float32)
    perm_ref[...] = perm
    perm16 = perm.astype(jnp.bfloat16)
    one_row = subject_ref[...]
    starts = [jnp.sum((one_row < s).astype(jnp.float32)).astype(jnp.int32) for s in range(SUBJ + 1)]
    place = lax.broadcasted_iota(jnp.int32, (epochs, LANES), 0)
    sid = jnp.zeros((epochs, LANES), jnp.int32)
    for s in range(1, SUBJ):
        sid = sid + (place >= starts[s]).astype(jnp.int32)
    sid_ref[...] = sid

    def arrange(t, carry):
        sorted_ref[t] = jnp.dot(perm16, ext_ref[t], preferred_element_type=jnp.float32)
        return carry

    lax.fori_loop(0, points, arrange, 0)

    blank = jnp.zeros((LANES - depth, block_len), jnp.float32)

    def fill(g, carry):
        cells = normalized(sorted_ref[:, pl.ds(pl.multiple_of(g * GROUP, GROUP), GROUP), :])
        cells = cells.reshape(depth, wide)
        base = pl.multiple_of(g * depth, depth)
        for side in range(2):
            win_ref[side, pl.ds(base, depth), :] = cells[:, side * CHUNK:side * CHUNK + span].astype(jnp.bfloat16)
        own = cells[:, LEAD:LEAD + block_len].astype(jnp.bfloat16).astype(jnp.float32)
        flat = jnp.concatenate([own, blank], axis=0).T
        for b in range(block_len // ROWS):
            piece = flat[b * ROWS:(b + 1) * ROWS, :]
            own_ref[b, g] = jnp.concatenate([piece, piece], axis=0).astype(jnp.bfloat16)
        return carry

    lax.fori_loop(0, groups, fill, 0)

    for half in range(block_len // LANES):
        at = idx_ref[:, half * LANES:(half + 1) * LANES].T
        centre = lax.broadcasted_iota(jnp.int32, (LANES, slots), 0) + half * LANES
        offset = at - (block_len - LEAD) - centre // CHUNK * CHUNK
        part = slice(half * LANES, (half + 1) * LANES)
        valid_ref[part, :] = (at >= 0).astype(jnp.float32)
        lane_ref[part, :] = jnp.where(at >= 0, offset & (LANES - 1), 0)
        tile_ref[part, :] = jnp.where(at >= 0, offset >> 7, 0)

    total_ref[...] = jnp.zeros_like(total_ref)
    masks = []
    for p in range(GROUP // 2):
        which = lax.broadcasted_iota(jnp.int32, (2 * ROWS, LANES), 0) // ROWS + 2 * p
        lane = lax.broadcasted_iota(jnp.int32, (2 * ROWS, LANES), 1) % GROUP
        masks.append((which == lane).astype(jnp.float32).astype(jnp.bfloat16))
    inverse = [1.0 / jnp.maximum((starts[s + 1] - starts[s]).astype(jnp.float32), 1.0) for s in range(SUBJ)]
    for sum_ref, sq_ref in ((sum0_ref, sq0_ref), (sum1_ref, sq1_ref)):
        sum_ref[0] = jnp.zeros((ROWS, LANES), jnp.float32)
        sq_ref[0] = jnp.zeros((ROWS, LANES), jnp.float32)

    def correlate(b, refs):
        x_ref, sum_ref, sq_ref = refs[:3]
        chunk = b // (CHUNK // ROWS)
        start = pl.multiple_of((chunk // 2) * LANES, LANES)
        here = pl.ds(pl.multiple_of(b * ROWS, ROWS), ROWS)
        lane = lane_ref[here, :]
        tile = tile_ref[here, :]
        first = tile == 0
        second = tile == 1
        running = jnp.zeros((ROWS, LANES), jnp.float32)
        squares = jnp.zeros((ROWS, LANES), jnp.float32)
        for g in range(groups):
            rhs = win_ref[lax.rem(chunk, 2), g * depth:(g + 1) * depth, pl.ds(start, SPAN)]
            own = own_ref[b, g]
            lhs = jnp.concatenate([own * m for m in masks], axis=0)[:, :depth]
            prod = jnp.dot(lhs, rhs, preferred_element_type=jnp.float32)
            for e in range(GROUP):
                r = e * ROWS
                parts = [take(prod[r:r + ROWS, t * LANES:(t + 1) * LANES], lane, BY_LANE)
                         for t in range(SPAN // LANES)]
                x = jnp.where(first, parts[0], jnp.where(second, parts[1], parts[2]))
                i = g * GROUP + e
                x_ref[i * ROWS:(i + 1) * ROWS, :] = x
                running = running + x
                squares = squares + x * x
                sum_ref[i + 1] = running
                sq_ref[i + 1] = squares

    def kernels(b, refs):
        x_ref, sum_ref, sq_ref, mean_ref, scale_ref = refs
        valid = valid_ref[pl.ds(pl.multiple_of(b * ROWS, ROWS), ROWS), :]
        for s in range(SUBJ):
            mean = (sum_ref[starts[s + 1]] - sum_ref[starts[s]]) * inverse[s]
            second = (sq_ref[starts[s + 1]] - sq_ref[starts[s]]) * inverse[s]
            var = jnp.maximum(second - mean * mean, 0.0)
            mean_ref[s * ROWS:(s + 1) * ROWS, :] = mean
            scale_ref[s * ROWS:(s + 1) * ROWS, :] = lax.rsqrt(var + VARIANCE_FLOOR) * valid
        acc = None
        for r in range(ROWS):
            mean = mean_ref[pl.ds(r, SUBJ, stride=ROWS), :]
            scale = scale_ref[pl.ds(r, SUBJ, stride=ROWS), :]
            pieces = []
            for q in range(epochs // 8):
                at = sid_ref[q * 8:(q + 1) * 8, :]
                x = x_ref[pl.ds(q * 8 * ROWS + r, 8, stride=ROWS), :]
                pieces.append((x - take(mean, at, BY_ROW)) * take(scale, at, BY_ROW))
            feat = jnp.concatenate(pieces, axis=0).astype(jnp.bfloat16)
            kern = lax.dot_general(feat, feat, (((1,), (1,)), ((), ())), preferred_element_type=jnp.float32)
            part = jnp.sum((kern * kern).reshape(epochs // 8, 8, epochs), axis=0)
            square_ref[pl.ds(pl.multiple_of((b * ROWS + r) * 8, 8), 8), :] = part
            acc = kern if acc is None else acc + kern
        total_ref[...] += acc

    even = (x0_ref, sum0_ref, sq0_ref, mean0_ref, scale0_ref)
    odd = (x1_ref, sum1_ref, sq1_ref, mean1_ref, scale1_ref)
    blocks = block_len // ROWS

    correlate(0, even)

    def two_blocks(j, carry):
        b = 2 * j
        kernels(b, even)
        correlate(b + 1, odd)
        kernels(b + 1, odd)
        correlate(jnp.minimum(b + 2, blocks - 1), even)
        return carry

    lax.fori_loop(0, blocks // 2, two_blocks, 0)

    for half in range(block_len // LANES):
        sums = None
        for r in range(8):
            part = square_ref[pl.ds(half * LANES * 8 + r, LANES, stride=8), :]
            sums = part if sums is None else sums + part
        sums = jnp.sum(sums.T, axis=0, keepdims=True)
        spread_ref[half:half + 1, :] = jnp.sqrt(sums * (1.0 / (epochs * NB * NB)))
    exact = lax.Precision.HIGHEST
    half_way = jnp.dot(total_ref[...], perm_ref[...], precision=exact, preferred_element_type=jnp.float32)
    gram_ref[...] = jnp.dot(perm_ref[...].T, half_way, precision=exact, preferred_element_type=jnp.float32)


def sum_kernel(count, scale, part_ref, out_ref, took, send1, recv1, send2, recv2):
    me = lax.axis_index("bx")
    barrier = pltpu.get_barrier_semaphore()

    def greet(d, carry):
        pl.semaphore_signal(barrier, inc=1, device_id={"bx": lax.rem(me + d, count)}, device_id_type=MESH)
        return carry

    lax.fori_loop(1, count, greet, 0)
    pl.semaphore_wait(barrier, count - 1)

    def scatter(d):
        to = lax.rem(me + d, count)
        return pltpu.make_async_remote_copy(
            src_ref=part_ref.at[to], dst_ref=took.at[d], send_sem=send1.at[d], recv_sem=recv1.at[d],
            device_id={"bx": to}, device_id_type=MESH)

    def gather(d):
        return pltpu.make_async_remote_copy(
            src_ref=out_ref.at[me], dst_ref=out_ref.at[me], send_sem=send2.at[d], recv_sem=recv2.at[d],
            device_id={"bx": lax.rem(me + d, count)}, device_id_type=MESH)

    def landed(d):
        src = lax.rem(me + count - d, count)
        return pltpu.make_async_remote_copy(
            src_ref=out_ref.at[src], dst_ref=out_ref.at[src], send_sem=send2.at[d], recv_sem=recv2.at[d],
            device_id={"bx": lax.rem(me + d, count)}, device_id_type=MESH)

    def each(act):
        def body(d, carry):
            act(d)
            return carry
        lax.fori_loop(1, count, body, 0)

    each(lambda d: scatter(d).start())
    each(lambda d: scatter(d).wait_recv())

    def add(d, total):
        return total + took[d]

    out_ref[me] = lax.fori_loop(1, count, add, part_ref[me]) * scale
    each(lambda d: gather(d).start())
    each(lambda d: landed(d).wait_recv())
    each(lambda d: scatter(d).wait_send())
    each(lambda d: gather(d).wait_send())


def sum_over_bx(total, scale):
    count = lax.axis_size("bx")
    rows, cols = total.shape
    blocks = total.reshape(count, rows // count, cols)
    vmem = pl.BlockSpec(memory_space=pltpu.VMEM)
    return pl.pallas_call(
        functools.partial(sum_kernel, count, scale),
        in_specs=[vmem],
        out_specs=vmem,
        out_shape=jax.ShapeDtypeStruct(blocks.shape, jnp.float32),
        scratch_shapes=[pltpu.VMEM(blocks.shape, jnp.float32)] + [pltpu.SemaphoreType.DMA((count,))] * 4,
        compiler_params=pltpu.CompilerParams(collective_id=0, has_side_effects=True),
        name="sum_over_bx",
    )(blocks).reshape(rows, cols)


def per_device(bold, nbr_table, subject):
    epochs, points, block_len = bold.shape
    slots = nbr_table.shape[0]
    count = lax.axis_size("bx")
    bold = bold.transpose(1, 0, 2)
    left = lax.ppermute(bold[:, :, block_len - LEAD:], "bx", [(i, i + 1) for i in range(count - 1)])
    right = lax.ppermute(bold[:, :, :LEAD], "bx", [(i + 1, i) for i in range(count - 1)])
    vmem = pl.BlockSpec(memory_space=pltpu.VMEM)
    ext = jnp.concatenate([left, bold, right], axis=2)
    wide = ext.shape[2]
    groups = epochs // GROUP
    f32 = functools.partial(pltpu.VMEM, dtype=jnp.float32)
    spread, total = pl.pallas_call(
        features_kernel,
        in_specs=[vmem] * 3,
        out_specs=[vmem] * 2,
        out_shape=[jax.ShapeDtypeStruct((block_len // LANES, LANES), jnp.float32),
                   jax.ShapeDtypeStruct((epochs, epochs), jnp.float32)],
        scratch_shapes=[
            f32((points, epochs, wide)),
            pltpu.VMEM((2, points * epochs, SPAN + LANES), jnp.bfloat16),
            pltpu.VMEM((block_len // ROWS, groups, 2 * ROWS, LANES), jnp.bfloat16),
            pltpu.VMEM((block_len, slots), jnp.int32),
            pltpu.VMEM((block_len, slots), jnp.int32),
            f32((block_len, slots)),
            pltpu.VMEM((epochs, LANES), jnp.int32),
            f32((epochs, epochs)),
            *[f32((epochs * ROWS, LANES))] * 2,
            *[f32((epochs + 1, ROWS, LANES))] * 4,
            *[f32((SUBJ * ROWS, LANES))] * 4,
            f32((block_len * 8, epochs)),
            f32((epochs, epochs)),
        ],
        compiler_params=pltpu.CompilerParams(vmem_limit_bytes=60 * 1024 * 1024),
        name="features",
    )(ext, nbr_table, subject[None, :])
    gram_mean = sum_over_bx(total, 1.0 / (NB * block_len * count))
    return spread.reshape(block_len), gram_mean


def solution(mesh):
    return jax.shard_map(
        per_device,
        mesh=mesh,
        in_specs=(P("cohort", None, "bx"), P("cohort", "bx"), P("cohort")),
        out_specs=(P(("cohort", "bx")), P("cohort", None)),
        check_vma=False,
    )
```

```python
import functools

import jax
import jax.numpy as jnp
from jax import lax
from jax.experimental import pallas as pl
from jax.experimental.pallas import tpu as pltpu
from jax.sharding import PartitionSpec as P

NB = 125
SUBJ = 8
REACH = 147
VARIANCE_FLOOR = 0.05

LANES = 128
ROWS = 8
GROUP = 8
CHUNK = 64
LEAD = 160
SPAN = 384
MESH = pl.DeviceIdType.MESH
BY_ROW = lax.GatherDimensionNumbers(
    offset_dims=(), collapsed_slice_dims=(0,), start_index_map=(0,),
    operand_batching_dims=(1,), start_indices_batching_dims=(1,))
BY_LANE = lax.GatherDimensionNumbers(
    offset_dims=(), collapsed_slice_dims=(1,), start_index_map=(1,),
    operand_batching_dims=(0,), start_indices_batching_dims=(0,))


def take(values, at, dims):
    return lax.gather(values, at[..., None], dims, (1, 1), mode="promise_in_bounds")


def normalized(values):
    points = values.shape[0]
    centred = values - jnp.sum(values, axis=0, keepdims=True) * (1.0 / points)
    return centred * (1.0 / jnp.sqrt(jnp.sum(centred * centred, axis=0, keepdims=True) + 1.0))


def reduce_over_bx(count, scale, part_ref, out_ref, took, send1, recv1, send2, recv2):
    me = lax.axis_index("bx")
    rows = out_ref.shape[0] // count

    def block(i):
        return pl.ds(pl.multiple_of(i * rows, rows), rows)

    def scatter(d):
        to = lax.rem(me + d, count)
        return pltpu.make_async_remote_copy(
            src_ref=part_ref.at[block(to)], dst_ref=took.at[d], send_sem=send1.at[d], recv_sem=recv1.at[d],
            device_id={"bx": to}, device_id_type=MESH)

    def gather(d):
        return pltpu.make_async_remote_copy(
            src_ref=out_ref.at[block(me)], dst_ref=out_ref.at[block(me)], send_sem=send2.at[d], recv_sem=recv2.at[d],
            device_id={"bx": lax.rem(me + d, count)}, device_id_type=MESH)

    def landed(d):
        src = lax.rem(me + count - d, count)
        return pltpu.make_async_remote_copy(
            src_ref=out_ref.at[block(src)], dst_ref=out_ref.at[block(src)], send_sem=send2.at[d], recv_sem=recv2.at[d],
            device_id={"bx": lax.rem(me + d, count)}, device_id_type=MESH)

    def each(act):
        def body(d, carry):
            act(d)
            return carry
        lax.fori_loop(1, count, body, 0)

    each(lambda d: scatter(d).start())
    each(lambda d: scatter(d).wait_recv())

    def add(d, total):
        return total + took[d]

    out_ref[block(me), :] = lax.fori_loop(1, count, add, part_ref[block(me), :]) * scale
    each(lambda d: gather(d).start())
    each(lambda d: landed(d).wait_recv())
    each(lambda d: scatter(d).wait_send())
    each(lambda d: gather(d).wait_send())


def greet_bx(count):
    me = lax.axis_index("bx")
    barrier = pltpu.get_barrier_semaphore()

    def greet(d, carry):
        pl.semaphore_signal(barrier, inc=1, device_id={"bx": lax.rem(me + d, count)}, device_id_type=MESH)
        return carry

    lax.fori_loop(1, count, greet, 0)


def features_kernel(count, ext_ref, idx_ref, subject_ref, spread_ref, gram_ref,
                    sorted_ref, win_ref, own_ref, lane_ref, tile_ref, valid_ref, sid_ref, perm_ref,
                    x0_ref, x1_ref, sum0_ref, sum1_ref, sq0_ref, sq1_ref, mean0_ref, mean1_ref,
                    scale0_ref, scale1_ref, square_ref, total_ref,
                    took_ref, send1, recv1, send2, recv2):
    points, epochs, wide = ext_ref.shape
    slots, block_len = idx_ref.shape
    groups = epochs // GROUP
    depth = points * GROUP
    span = SPAN + LANES

    greet_bx(count)
    named = jnp.broadcast_to(subject_ref[...], (epochs, LANES))
    named_t = named.T
    row = lax.broadcasted_iota(jnp.int32, (epochs, LANES), 0)
    col = lax.broadcasted_iota(jnp.int32, (epochs, LANES), 1)
    ahead = (named_t < named) | ((named_t == named) & (row < col))
    rank = jnp.sum(ahead.astype(jnp.float32), axis=0, keepdims=True).astype(jnp.int32)
    perm = (jnp.broadcast_to(rank, (epochs, LANES)) == row).astype(jnp.float32)
    perm_ref[...] = perm
    perm16 = perm.astype(jnp.bfloat16)
    one_row = subject_ref[...]
    starts = [jnp.clip(jnp.sum((one_row < s).astype(jnp.float32)).astype(jnp.int32), 0, epochs)
              for s in range(SUBJ + 1)]
    place = lax.broadcasted_iota(jnp.int32, (epochs, LANES), 0)
    sid = jnp.zeros((epochs, LANES), jnp.int32)
    for s in range(1, SUBJ):
        sid = sid + (place >= starts[s]).astype(jnp.int32)
    sid_ref[...] = sid

    def arrange(t, carry):
        sorted_ref[t] = jnp.dot(perm16, ext_ref[t], preferred_element_type=jnp.float32)
        return carry

    lax.fori_loop(0, points, arrange, 0)

    blank = jnp.zeros((LANES - depth, block_len), jnp.float32)

    def fill(g, carry):
        cells = normalized(sorted_ref[:, pl.ds(pl.multiple_of(g * GROUP, GROUP), GROUP), :])
        cells = cells.reshape(depth, wide)
        base = pl.multiple_of(g * depth, depth)
        for side in range(2):
            win_ref[side, pl.ds(base, depth), :] = cells[:, side * CHUNK:side * CHUNK + span].astype(jnp.bfloat16)
        own = cells[:, LEAD:LEAD + block_len].astype(jnp.bfloat16).astype(jnp.float32)
        flat = jnp.concatenate([own, blank], axis=0).T
        for b in range(block_len // ROWS):
            piece = flat[b * ROWS:(b + 1) * ROWS, :]
            own_ref[b, g] = jnp.concatenate([piece, piece], axis=0).astype(jnp.bfloat16)
        return carry

    lax.fori_loop(0, groups, fill, 0)

    for half in range(block_len // LANES):
        at = idx_ref[:, half * LANES:(half + 1) * LANES].T
        centre = lax.broadcasted_iota(jnp.int32, (LANES, slots), 0) + half * LANES
        offset = at - (block_len - LEAD) - centre // CHUNK * CHUNK
        part = slice(half * LANES, (half + 1) * LANES)
        valid_ref[part, :] = (at >= 0).astype(jnp.float32)
        lane_ref[part, :] = jnp.where(at >= 0, offset & (LANES - 1), 0)
        tile_ref[part, :] = jnp.where(at >= 0, offset >> 7, 0)

    total_ref[...] = jnp.zeros_like(total_ref)
    masks = []
    for p in range(GROUP // 2):
        which = lax.broadcasted_iota(jnp.int32, (2 * ROWS, LANES), 0) // ROWS + 2 * p
        lane = lax.broadcasted_iota(jnp.int32, (2 * ROWS, LANES), 1) % GROUP
        masks.append((which == lane).astype(jnp.float32).astype(jnp.bfloat16))
    inverse = [1.0 / jnp.maximum((starts[s + 1] - starts[s]).astype(jnp.float32), 1.0) for s in range(SUBJ)]
    for sum_ref, sq_ref in ((sum0_ref, sq0_ref), (sum1_ref, sq1_ref)):
        sum_ref[0] = jnp.zeros((ROWS, LANES), jnp.float32)
        sq_ref[0] = jnp.zeros((ROWS, LANES), jnp.float32)

    def correlate(b, refs):
        x_ref, sum_ref, sq_ref = refs[:3]
        chunk = b // (CHUNK // ROWS)
        start = pl.multiple_of((chunk // 2) * LANES, LANES)
        here = pl.ds(pl.multiple_of(b * ROWS, ROWS), ROWS)
        lane = lane_ref[here, :]
        tile = tile_ref[here, :]
        first = tile == 0
        second = tile == 1
        running = jnp.zeros((ROWS, LANES), jnp.float32)
        squares = jnp.zeros((ROWS, LANES), jnp.float32)
        for g in range(groups):
            rhs = win_ref[lax.rem(chunk, 2), g * depth:(g + 1) * depth, pl.ds(start, SPAN)]
            own = own_ref[b, g]
            lhs = jnp.concatenate([own * m for m in masks], axis=0)[:, :depth]
            prod = jnp.dot(lhs, rhs, preferred_element_type=jnp.float32)
            for e in range(GROUP):
                r = e * ROWS
                parts = [take(prod[r:r + ROWS, t * LANES:(t + 1) * LANES], lane, BY_LANE)
                         for t in range(SPAN // LANES)]
                x = jnp.where(first, parts[0], jnp.where(second, parts[1], parts[2]))
                i = g * GROUP + e
                x_ref[i * ROWS:(i + 1) * ROWS, :] = x
                running = running + x
                squares = squares + x * x
                sum_ref[i + 1] = running
                sq_ref[i + 1] = squares
            yield

    def kernels(b, refs):
        x_ref, sum_ref, sq_ref, mean_ref, scale_ref = refs
        valid = valid_ref[pl.ds(pl.multiple_of(b * ROWS, ROWS), ROWS), :]
        for s in range(SUBJ):
            mean = (sum_ref[starts[s + 1]] - sum_ref[starts[s]]) * inverse[s]
            second = (sq_ref[starts[s + 1]] - sq_ref[starts[s]]) * inverse[s]
            var = jnp.maximum(second - mean * mean, 0.0)
            mean_ref[s * ROWS:(s + 1) * ROWS, :] = mean
            scale_ref[s * ROWS:(s + 1) * ROWS, :] = lax.rsqrt(var + VARIANCE_FLOOR) * valid
        acc = None
        for r in range(ROWS):
            mean = mean_ref[pl.ds(r, SUBJ, stride=ROWS), :]
            scale = scale_ref[pl.ds(r, SUBJ, stride=ROWS), :]
            pieces = []
            for q in range(epochs // 8):
                at = sid_ref[q * 8:(q + 1) * 8, :]
                x = x_ref[pl.ds(q * 8 * ROWS + r, 8, stride=ROWS), :]
                pieces.append((x - take(mean, at, BY_ROW)) * take(scale, at, BY_ROW))
            feat = jnp.concatenate(pieces, axis=0).astype(jnp.bfloat16)
            kern = lax.dot_general(feat, feat, (((1,), (1,)), ((), ())), preferred_element_type=jnp.float32)
            part = jnp.sum((kern * kern).reshape(epochs // 8, 8, epochs), axis=0)
            square_ref[pl.ds(pl.multiple_of((b * ROWS + r) * 8, 8), 8), :] = part
            acc = kern if acc is None else acc + kern
            yield
        total_ref[...] += acc

    even = (x0_ref, sum0_ref, sq0_ref, mean0_ref, scale0_ref)
    odd = (x1_ref, sum1_ref, sq1_ref, mean1_ref, scale1_ref)
    blocks = block_len // ROWS

    def together(first, second):
        pace = groups // ROWS
        for _ in range(ROWS):
            for _ in range(pace):
                next(first)
            next(second)
        for rest in (first, second):
            for _ in rest:
                pass

    for _ in correlate(0, even):
        pass

    def two_blocks(j, carry):
        b = 2 * j
        together(correlate(b + 1, odd), kernels(b, even))
        together(correlate(jnp.minimum(b + 2, blocks - 1), even), kernels(b + 1, odd))
        return carry

    lax.fori_loop(0, blocks // 2, two_blocks, 0)

    for half in range(block_len // LANES):
        sums = None
        for r in range(8):
            part = square_ref[pl.ds(half * LANES * 8 + r, LANES, stride=8), :]
            sums = part if sums is None else sums + part
        sums = jnp.sum(sums.T, axis=0, keepdims=True)
        spread_ref[half:half + 1, :] = jnp.sqrt(sums * (1.0 / (epochs * NB * NB)))
    exact = lax.Precision.HIGHEST
    half_way = jnp.dot(total_ref[...], perm_ref[...], precision=exact, preferred_element_type=jnp.float32)
    total_ref[...] = jnp.dot(perm_ref[...].T, half_way, precision=exact, preferred_element_type=jnp.float32)
    pl.semaphore_wait(pltpu.get_barrier_semaphore(), count - 1)
    reduce_over_bx(count, 1.0 / (NB * block_len * count), total_ref, gram_ref, took_ref, send1, recv1, send2, recv2)


def per_device(bold, nbr_table, subject):
    epochs, points, block_len = bold.shape
    slots = nbr_table.shape[0]
    count = lax.axis_size("bx")
    bold = bold.transpose(1, 0, 2)
    left = lax.ppermute(bold[:, :, block_len - LEAD:], "bx", [(i, i + 1) for i in range(count - 1)])
    right = lax.ppermute(bold[:, :, :LEAD], "bx", [(i + 1, i) for i in range(count - 1)])
    vmem = pl.BlockSpec(memory_space=pltpu.VMEM)
    ext = jnp.concatenate([left, bold, right], axis=2)
    wide = ext.shape[2]
    groups = epochs // GROUP
    f32 = functools.partial(pltpu.VMEM, dtype=jnp.float32)
    spread, gram_mean = pl.pallas_call(
        functools.partial(features_kernel, count),
        in_specs=[vmem] * 3,
        out_specs=[vmem] * 2,
        out_shape=[jax.ShapeDtypeStruct((block_len // LANES, LANES), jnp.float32),
                   jax.ShapeDtypeStruct((epochs, epochs), jnp.float32)],
        scratch_shapes=[
            f32((points, epochs, wide)),
            pltpu.VMEM((2, points * epochs, SPAN + LANES), jnp.bfloat16),
            pltpu.VMEM((block_len // ROWS, groups, 2 * ROWS, LANES), jnp.bfloat16),
            pltpu.VMEM((block_len, slots), jnp.int32),
            pltpu.VMEM((block_len, slots), jnp.int32),
            f32((block_len, slots)),
            pltpu.VMEM((epochs, LANES), jnp.int32),
            f32((epochs, epochs)),
            *[f32((epochs * ROWS, LANES))] * 2,
            *[f32((epochs + 1, ROWS, LANES))] * 4,
            *[f32((SUBJ * ROWS, LANES))] * 4,
            f32((block_len * 8, epochs)),
            f32((epochs, epochs)),
            f32((count, epochs // count, epochs)),
            *[pltpu.SemaphoreType.DMA((count,))] * 4,
        ],
        compiler_params=pltpu.CompilerParams(collective_id=0, has_side_effects=True,
                                             vmem_limit_bytes=60 * 1024 * 1024),
        name="features",
    )(ext, nbr_table, subject[None, :])
    return spread.reshape(block_len), gram_mean


def solution(mesh):
    return jax.shard_map(
        per_device,
        mesh=mesh,
        in_specs=(P("cohort", None, "bx"), P("cohort", "bx"), P("cohort")),
        out_specs=(P(("cohort", "bx")), P("cohort", None)),
        check_vma=False,
    )
```

```python
import functools

import jax
import jax.numpy as jnp
from jax import lax
from jax.experimental import pallas as pl
from jax.experimental.pallas import tpu as pltpu
from jax.sharding import PartitionSpec as P

NB = 125
SUBJ = 8
REACH = 147
VARIANCE_FLOOR = 0.05

LANES = 128
ROWS = 8
GROUP = 8
AHEAD = 5
HALF = 64
SPAN = 384
NEAR, FAR, EDGE = range(3)
MESH = pl.DeviceIdType.MESH
BY_ROW = lax.GatherDimensionNumbers(
    offset_dims=(), collapsed_slice_dims=(0,), start_index_map=(0,),
    operand_batching_dims=(1,), start_indices_batching_dims=(1,))
BY_LANE = lax.GatherDimensionNumbers(
    offset_dims=(), collapsed_slice_dims=(1,), start_index_map=(1,),
    operand_batching_dims=(0,), start_indices_batching_dims=(0,))


def take(values, at, dims):
    return lax.gather(values, at[..., None], dims, (1, 1), mode="promise_in_bounds")


def normalized(values):
    points = values.shape[0]
    centred = values - jnp.sum(values, axis=0, keepdims=True) * (1.0 / points)
    return centred * (1.0 / jnp.sqrt(jnp.sum(centred * centred, axis=0, keepdims=True) + 1.0))


def reduce_over_bx(count, scale, part_ref, out_ref, took, send1, recv1, send2, recv2):
    me = lax.axis_index("bx")
    rows = out_ref.shape[0] // count

    def block(i):
        return pl.ds(pl.multiple_of(i * rows, rows), rows)

    def scatter(d):
        to = lax.rem(me + d, count)
        return pltpu.make_async_remote_copy(
            src_ref=part_ref.at[block(to)], dst_ref=took.at[d], send_sem=send1.at[d], recv_sem=recv1.at[d],
            device_id={"bx": to}, device_id_type=MESH)

    def gather(d):
        return pltpu.make_async_remote_copy(
            src_ref=out_ref.at[block(me)], dst_ref=out_ref.at[block(me)], send_sem=send2.at[d], recv_sem=recv2.at[d],
            device_id={"bx": lax.rem(me + d, count)}, device_id_type=MESH)

    def landed(d):
        src = lax.rem(me + count - d, count)
        return pltpu.make_async_remote_copy(
            src_ref=out_ref.at[block(src)], dst_ref=out_ref.at[block(src)], send_sem=send2.at[d], recv_sem=recv2.at[d],
            device_id={"bx": lax.rem(me + d, count)}, device_id_type=MESH)

    def each(act):
        def body(d, carry):
            act(d)
            return carry
        lax.fori_loop(1, count, body, 0)

    each(lambda d: scatter(d).start())
    each(lambda d: scatter(d).wait_recv())

    def add(d, total):
        return total + took[d]

    out_ref[block(me), :] = lax.fori_loop(1, count, add, part_ref[block(me), :]) * scale
    each(lambda d: gather(d).start())
    each(lambda d: landed(d).wait_recv())
    each(lambda d: scatter(d).wait_send())
    each(lambda d: gather(d).wait_send())


def greet_bx(count):
    me = lax.axis_index("bx")
    barrier = pltpu.get_barrier_semaphore()

    def greet(d, carry):
        pl.semaphore_signal(barrier, inc=1, device_id={"bx": lax.rem(me + d, count)}, device_id_type=MESH)
        return carry

    lax.fori_loop(1, count, greet, 0)


def plan_blocks(block_len):
    windows = ((NEAR, -HALF, 5 * LANES), (FAR, -LANES, 0), (FAR, 0, LANES),
               (EDGE, -LANES - HALF, 4 * LANES), (EDGE, HALF, 6 * LANES))
    left = list(range(block_len // ROWS))
    runs = []
    for phase, column, lane in windows:
        fits = [b for b in left if column <= b * ROWS - REACH and b * ROWS + ROWS + REACH <= column + SPAN]
        left = [b for b in left if b not in fits]
        runs.append((phase, len(fits), fits[0], column, lane))
        assert fits == list(range(fits[0], fits[0] + len(fits)))
    assert not left and block_len == 2 * LANES
    return runs


def pick(value, runs):
    result = runs[-1][1]
    for bound, entry in runs[-2::-1]:
        result = jnp.where(value < bound, entry, result)
    return result


def features_kernel(count, bold_ref, idx_ref, subject_ref, spread_ref, gram_ref,
                    sorted_ref, win_ref, quarter_ref, halo_ref, own_ref, lane_ref, tile_ref, valid_ref,
                    sid_ref, perm_ref, x0_ref, x1_ref, sum0_ref, sum1_ref, sq0_ref, sq1_ref,
                    mean0_ref, mean1_ref, scale0_ref, scale1_ref, square_ref, total_ref, prod_ref,
                    took_ref, send0, recv0, send1, recv1, send2, recv2):
    points, epochs, block_len = bold_ref.shape
    slots = idx_ref.shape[0]
    groups = epochs // GROUP
    depth = points * GROUP
    packed = points * epochs // 2
    me = lax.axis_index("bx")
    runs = plan_blocks(block_len)
    ends = [sum(r[1] for r in runs[:i + 1]) for i in range(len(runs))]

    greet_bx(count)
    named = jnp.broadcast_to(subject_ref[...], (epochs, LANES))
    named_t = named.T
    row = lax.broadcasted_iota(jnp.int32, (epochs, LANES), 0)
    col = lax.broadcasted_iota(jnp.int32, (epochs, LANES), 1)
    ahead = (named_t < named) | ((named_t == named) & (row < col))
    rank = jnp.sum(ahead.astype(jnp.float32), axis=0, keepdims=True).astype(jnp.int32)
    perm = (jnp.broadcast_to(rank, (epochs, LANES)) == row).astype(jnp.float32)
    perm_ref[...] = perm
    perm16 = perm.astype(jnp.bfloat16)

    def arrange(t, carry):
        sorted_ref[t] = jnp.dot(perm16, bold_ref[t], preferred_element_type=jnp.float32)
        return carry

    lax.fori_loop(0, points, arrange, 0)

    blank = jnp.zeros((LANES - depth, block_len), jnp.float32)

    def tile_of(i):
        return slice(i * LANES, (i + 1) * LANES)

    def join(low, high):
        return jnp.concatenate([low, high], axis=1)

    def turned(values):
        return join(values[:, HALF:], values[:, :HALF])

    def fill(g, carry):
        cells = normalized(sorted_ref[:, pl.ds(pl.multiple_of(g * GROUP, GROUP), GROUP), :])
        cells = cells.reshape(depth, block_len).astype(jnp.bfloat16)
        rows = pl.ds(pl.multiple_of(g * depth, depth), depth)
        here0, here1 = cells[:, :LANES], cells[:, LANES:]
        turn0, turn1 = turned(here0), turned(here1)
        win_ref[rows, tile_of(1)] = here0
        win_ref[rows, tile_of(2)] = here1
        win_ref[rows, tile_of(5)] = turn0
        win_ref[rows, tile_of(6)] = join(turn0[:, :HALF], turn1[:, HALF:])
        win_ref[rows, tile_of(7)] = turn1
        return carry

    lax.fori_loop(0, groups, fill, 0)

    def pair_rows(g):
        first = pl.multiple_of(g * depth, depth)
        return pl.ds(first, depth), pl.ds(pl.multiple_of(first + packed, depth), depth)

    def pack(g, carry):
        upper, lower = pair_rows(g)
        for q, straight in enumerate((1, None, 2, None)):
            here, turn = ((1, 5), (1, 5), (2, 7), (2, 7))[q]
            one, two = (here, turn) if straight else (turn, here)
            quarter_ref[q, upper, :] = join(win_ref[upper, tile_of(one)][:, :HALF], win_ref[lower, tile_of(two)][:, HALF:])
        return carry

    lax.fori_loop(0, groups // 2, pack, 0)

    pl.semaphore_wait(pltpu.get_barrier_semaphore(), count - 1)

    def message(side, phase):
        quarter = (3 - phase) if side == 0 else phase
        to = me + 1 if side == 0 else me - 1
        return pltpu.make_async_remote_copy(
            src_ref=quarter_ref.at[quarter], dst_ref=halo_ref.at[side * 3 + phase],
            send_sem=send0.at[side * 3 + phase], recv_sem=recv0.at[side * 3 + phase],
            device_id={"bx": to}, device_id_type=MESH)

    sends = (me < count - 1, me > 0)
    gets = (me > 0, me < count - 1)
    for phase in range(3):
        for side in range(2):
            @pl.when(sends[side])
            def _():
                message(side, phase).start()

    for side in range(2):
        @pl.when(jnp.logical_not(gets[side]))
        def _():
            for phase in range(3):
                halo_ref[side * 3 + phase] = jnp.zeros((packed, LANES), jnp.bfloat16)

    one_row = subject_ref[...]
    starts = [jnp.clip(jnp.sum((one_row < s).astype(jnp.float32)).astype(jnp.int32), 0, epochs)
              for s in range(SUBJ + 1)]
    sid = jnp.zeros((epochs, LANES), jnp.int32)
    for s in range(1, SUBJ):
        sid = sid + (row >= starts[s]).astype(jnp.int32)
    sid_ref[...] = sid

    def turn_own(g, carry):
        rows = pl.ds(pl.multiple_of(g * depth, depth), depth)
        own = win_ref[rows, LANES:LANES + block_len].astype(jnp.float32)
        flat = jnp.concatenate([own, blank], axis=0).T
        for b in range(block_len // ROWS):
            piece = flat[b * ROWS:(b + 1) * ROWS, :]
            own_ref[b, g] = jnp.concatenate([piece, piece], axis=0).astype(jnp.bfloat16)
        return carry

    lax.fori_loop(0, groups, turn_own, 0)

    for half in range(block_len // LANES):
        at = idx_ref[:, half * LANES:(half + 1) * LANES].T
        centre = lax.broadcasted_iota(jnp.int32, (LANES, slots), 0) + half * LANES
        column = pick(centre // ROWS, sorted((r[2] + r[1], r[3]) for r in runs))
        offset = at - block_len - column
        part = slice(half * LANES, (half + 1) * LANES)
        valid_ref[part, :] = (at >= 0).astype(jnp.float32)
        lane_ref[part, :] = jnp.where(at >= 0, offset & (LANES - 1), 0)
        tile_ref[part, :] = jnp.where(at >= 0, offset >> 7, 0)

    def arrived(phase):
        for side in range(2):
            @pl.when(gets[side])
            def _():
                message(side, phase).wait_recv()

    def settle(phase):
        arrived(phase)
        left, right = halo_ref.at[phase], halo_ref.at[3 + phase]
        inner_left, inner_right = (halo_ref.at[phase - 1], halo_ref.at[2 + phase]) if phase else (None, None)

        def body(g, carry):
            upper, lower = pair_rows(g)
            near_l, near_r = left[upper, :], right[upper, :]
            if phase == NEAR:
                for rows, (l, r) in ((upper, (near_l, near_r[:, :HALF])), (lower, (near_l[:, HALF:], near_r[:, HALF:]))):
                    win_ref[rows, tile_of(5)] = join(l[:, :HALF], win_ref[rows, tile_of(5)][:, HALF:])
                    win_ref[rows, tile_of(7)] = join(win_ref[rows, tile_of(7)][:, :HALF], r)
            else:
                in_l, in_r = inner_left[upper, :], inner_right[upper, :]
                a, b = (0, 3) if phase == FAR else (4, 8)
                for rows, cut in ((upper, slice(0, HALF)), (lower, slice(HALF, LANES))):
                    win_ref[rows, tile_of(a)] = join(near_l[:, cut], in_l[:, cut])
                    win_ref[rows, tile_of(b)] = join(in_r[:, cut], near_r[:, cut])
            return carry

        lax.fori_loop(0, groups // 2, body, 0)

    total_ref[...] = jnp.zeros_like(total_ref)
    masks = []
    for p in range(GROUP // 2):
        which = lax.broadcasted_iota(jnp.int32, (2 * ROWS, LANES), 0) // ROWS + 2 * p
        lane = lax.broadcasted_iota(jnp.int32, (2 * ROWS, LANES), 1) % GROUP
        masks.append((which == lane).astype(jnp.float32).astype(jnp.bfloat16))
    inverse = [1.0 / jnp.maximum((starts[s + 1] - starts[s]).astype(jnp.float32), 1.0) for s in range(SUBJ)]
    for sum_ref, sq_ref in ((sum0_ref, sq0_ref), (sum1_ref, sq1_ref)):
        sum_ref[0] = jnp.zeros((ROWS, LANES), jnp.float32)
        sq_ref[0] = jnp.zeros((ROWS, LANES), jnp.float32)

    def nth(n):
        n = jnp.asarray(n, jnp.int32)
        block = n + pick(n, [(end, r[2] - (end - r[1])) for end, r in zip(ends, runs)])
        lane = pick(n, [(end, r[4]) for end, r in zip(ends, runs)])
        return block, pl.multiple_of(lane, LANES)

    def product(at, g):
        b, start = at
        rhs = win_ref[g * depth:(g + 1) * depth, pl.ds(start, SPAN)]
        own = own_ref[b, g]
        lhs = jnp.concatenate([own * m for m in masks], axis=0)[:, :depth]
        return jnp.dot(lhs, rhs, preferred_element_type=jnp.float32)

    def correlate(at, refs, queue, after):
        b = at[0]
        x_ref, sum_ref, sq_ref = refs[:3]
        here = pl.ds(pl.multiple_of(b * ROWS, ROWS), ROWS)
        lane = lane_ref[here, :]
        tile = tile_ref[here, :]
        first = tile == 0
        second = tile == 1
        running = jnp.zeros((ROWS, LANES), jnp.float32)
        squares = jnp.zeros((ROWS, LANES), jnp.float32)
        for g in range(groups):
            prod = queue.pop(0)
            for e in range(GROUP):
                r = e * ROWS
                parts = [take(prod[r:r + ROWS, t * LANES:(t + 1) * LANES], lane, BY_LANE)
                         for t in range(SPAN // LANES)]
                x = jnp.where(first, parts[0], jnp.where(second, parts[1], parts[2]))
                i = g * GROUP + e
                x_ref[i * ROWS:(i + 1) * ROWS, :] = x
                running = running + x
                squares = squares + x * x
                sum_ref[i + 1] = running
                sq_ref[i + 1] = squares
            ahead = g + AHEAD
            queue.append(product(at, ahead) if ahead < groups else product(after, ahead - groups))
            yield

    def kernels(b, refs):
        x_ref, sum_ref, sq_ref, mean_ref, scale_ref = refs
        valid = valid_ref[pl.ds(pl.multiple_of(b * ROWS, ROWS), ROWS), :]
        for s in range(SUBJ):
            mean = (sum_ref[starts[s + 1]] - sum_ref[starts[s]]) * inverse[s]
            second = (sq_ref[starts[s + 1]] - sq_ref[starts[s]]) * inverse[s]
            var = jnp.maximum(second - mean * mean, 0.0)
            mean_ref[s * ROWS:(s + 1) * ROWS, :] = mean
            scale_ref[s * ROWS:(s + 1) * ROWS, :] = lax.rsqrt(var + VARIANCE_FLOOR) * valid
        acc = None
        for r in range(ROWS):
            mean = mean_ref[pl.ds(r, SUBJ, stride=ROWS), :]
            scale = scale_ref[pl.ds(r, SUBJ, stride=ROWS), :]
            pieces = []
            for q in range(epochs // 8):
                at = sid_ref[q * 8:(q + 1) * 8, :]
                x = x_ref[pl.ds(q * 8 * ROWS + r, 8, stride=ROWS), :]
                pieces.append((x - take(mean, at, BY_ROW)) * take(scale, at, BY_ROW))
            feat = jnp.concatenate(pieces, axis=0).astype(jnp.bfloat16)
            kern = lax.dot_general(feat, feat, (((1,), (1,)), ((), ())), preferred_element_type=jnp.float32)
            part = jnp.sum((kern * kern).reshape(epochs // 8, 8, epochs), axis=0)
            square_ref[pl.ds(pl.multiple_of((b * ROWS + r) * 8, 8), 8), :] = part
            acc = kern if acc is None else acc + kern
            yield
        total_ref[...] += acc

    even = (x0_ref, sum0_ref, sq0_ref, mean0_ref, scale0_ref)
    odd = (x1_ref, sum1_ref, sq1_ref, mean1_ref, scale1_ref)
    blocks = block_len // ROWS

    def together(first, second):
        pace = groups // ROWS
        for _ in range(ROWS):
            for _ in range(pace):
                next(first)
            next(second)
        for rest in (first, second):
            for _ in rest:
                pass

    def keep(queue):
        for i, prod in enumerate(queue):
            prod_ref[i] = prod

    settle(NEAR)
    queue = [product(nth(0), g) for g in range(AHEAD)]
    for _ in correlate(nth(0), even, queue, nth(1)):
        pass
    keep(queue)
    near = sum(r[1] for r in runs if r[0] == NEAR)
    outer = sum(r[1] for r in runs if r[0] == EDGE)

    def two_blocks(j, carry):
        n = 2 * j

        @pl.when(j == (near - 3) // 2 + 1)
        def _():
            settle(FAR)

        @pl.when(j == (blocks - outer - 3) // 2 + 1)
        def _():
            settle(EDGE)

        queue = [prod_ref[i] for i in range(AHEAD)]
        last = nth(jnp.minimum(n + 2, blocks - 1))
        together(correlate(nth(n + 1), odd, queue, last), kernels(nth(n)[0], even))
        together(correlate(last, even, queue, nth(jnp.minimum(n + 3, blocks - 1))), kernels(nth(n + 1)[0], odd))
        keep(queue)
        return carry

    lax.fori_loop(0, blocks // 2, two_blocks, 0)

    for half in range(block_len // LANES):
        sums = None
        for r in range(8):
            part = square_ref[pl.ds(half * LANES * 8 + r, LANES, stride=8), :]
            sums = part if sums is None else sums + part
        sums = jnp.sum(sums.T, axis=0, keepdims=True)
        spread_ref[half:half + 1, :] = jnp.sqrt(sums * (1.0 / (epochs * NB * NB)))
    exact = lax.Precision.HIGHEST
    half_way = jnp.dot(total_ref[...], perm_ref[...], precision=exact, preferred_element_type=jnp.float32)
    total_ref[...] = jnp.dot(perm_ref[...].T, half_way, precision=exact, preferred_element_type=jnp.float32)
    for phase in range(3):
        for side in range(2):
            @pl.when(sends[side])
            def _():
                message(side, phase).wait_send()

    reduce_over_bx(count, 1.0 / (NB * block_len * count), total_ref, gram_ref, took_ref, send1, recv1, send2, recv2)


def per_device(bold, nbr_table, subject):
    epochs, points, block_len = bold.shape
    slots = nbr_table.shape[0]
    count = lax.axis_size("bx")
    bold = bold.transpose(1, 0, 2)
    vmem = pl.BlockSpec(memory_space=pltpu.VMEM)
    groups = epochs // GROUP
    f32 = functools.partial(pltpu.VMEM, dtype=jnp.float32)
    spread, gram_mean = pl.pallas_call(
        functools.partial(features_kernel, count),
        in_specs=[vmem] * 3,
        out_specs=[vmem] * 2,
        out_shape=[jax.ShapeDtypeStruct((block_len // LANES, LANES), jnp.float32),
                   jax.ShapeDtypeStruct((epochs, epochs), jnp.float32)],
        scratch_shapes=[
            f32((points, epochs, block_len)),
            pltpu.VMEM((points * epochs, 9 * LANES), jnp.bfloat16),
            pltpu.VMEM((4, points * epochs // 2, LANES), jnp.bfloat16),
            pltpu.VMEM((6, points * epochs // 2, LANES), jnp.bfloat16),
            pltpu.VMEM((block_len // ROWS, groups, 2 * ROWS, LANES), jnp.bfloat16),
            pltpu.VMEM((block_len, slots), jnp.int32),
            pltpu.VMEM((block_len, slots), jnp.int32),
            f32((block_len, slots)),
            pltpu.VMEM((epochs, LANES), jnp.int32),
            f32((epochs, epochs)),
            *[f32((epochs * ROWS, LANES))] * 2,
            *[f32((epochs + 1, ROWS, LANES))] * 4,
            *[f32((SUBJ * ROWS, LANES))] * 4,
            f32((block_len * 8, epochs)),
            f32((epochs, epochs)),
            f32((AHEAD, GROUP * ROWS, SPAN)),
            f32((count, epochs // count, epochs)),
            *[pltpu.SemaphoreType.DMA((6,))] * 2,
            *[pltpu.SemaphoreType.DMA((count,))] * 4,
        ],
        compiler_params=pltpu.CompilerParams(collective_id=0, has_side_effects=True,
                                             vmem_limit_bytes=60 * 1024 * 1024),
        name="features",
    )(bold, nbr_table, subject[None, :])
    return spread.reshape(block_len), gram_mean


def solution(mesh):
    return jax.shard_map(
        per_device,
        mesh=mesh,
        in_specs=(P("cohort", None, "bx"), P("cohort", "bx"), P("cohort")),
        out_specs=(P(("cohort", "bx")), P("cohort", None)),
        check_vma=False,
    )
```

```python
import functools

import jax
import jax.numpy as jnp
from jax import lax
from jax.experimental import pallas as pl
from jax.experimental.pallas import tpu as pltpu
from jax.sharding import PartitionSpec as P

NB = 125
SUBJ = 8
REACH = 147
VARIANCE_FLOOR = 0.05

LANES = 128
ROWS = 8
GROUP = 8
AHEAD = 5
HALF = 64
SPAN = 384
NEAR, FAR, EDGE = range(3)
MESH = pl.DeviceIdType.MESH
BY_ROW = lax.GatherDimensionNumbers(
    offset_dims=(), collapsed_slice_dims=(0,), start_index_map=(0,),
    operand_batching_dims=(1,), start_indices_batching_dims=(1,))
BY_LANE = lax.GatherDimensionNumbers(
    offset_dims=(), collapsed_slice_dims=(1,), start_index_map=(1,),
    operand_batching_dims=(0,), start_indices_batching_dims=(0,))


def take(values, at, dims):
    return lax.gather(values, at[..., None], dims, (1, 1), mode="promise_in_bounds")


def normalized(values):
    points = values.shape[0]
    centred = values - jnp.sum(values, axis=0, keepdims=True) * (1.0 / points)
    return centred * (1.0 / jnp.sqrt(jnp.sum(centred * centred, axis=0, keepdims=True) + 1.0))


def reduce_over_bx(count, scale, between, part_ref, out_ref, took, send1, recv1, send2, recv2):
    me = lax.axis_index("bx")
    rows = part_ref.shape[0] // count

    def block(i):
        return pl.ds(pl.multiple_of(i * rows, rows), rows)

    def scatter(d):
        to = lax.rem(me + d, count)
        return pltpu.make_async_remote_copy(
            src_ref=part_ref.at[block(to)], dst_ref=took.at[d], send_sem=send1.at[d], recv_sem=recv1.at[d],
            device_id={"bx": to}, device_id_type=MESH)

    def gather(d):
        return pltpu.make_async_remote_copy(
            src_ref=out_ref.at[block(me)], dst_ref=out_ref.at[block(me)], send_sem=send2.at[d], recv_sem=recv2.at[d],
            device_id={"bx": lax.rem(me + d, count)}, device_id_type=MESH)

    def landed(d):
        src = lax.rem(me + count - d, count)
        return pltpu.make_async_remote_copy(
            src_ref=out_ref.at[block(src)], dst_ref=out_ref.at[block(src)], send_sem=send2.at[d], recv_sem=recv2.at[d],
            device_id={"bx": lax.rem(me + d, count)}, device_id_type=MESH)

    def each(act):
        def body(d, carry):
            act(d)
            return carry
        if count <= 16:
            for d in range(1, count):
                act(d)
        else:
            lax.fori_loop(1, count, body, 0)

    each(lambda d: scatter(d).start())
    between()
    each(lambda d: scatter(d).wait_recv())

    def add(d, total):
        return total + took[d]

    out_ref[block(me), :] = lax.fori_loop(1, count, add, part_ref[block(me), :]) * scale
    each(lambda d: gather(d).start())
    each(lambda d: scatter(d).wait_send())
    each(lambda d: landed(d).wait_recv())
    each(lambda d: gather(d).wait_send())


def greet_bx(count):
    me = lax.axis_index("bx")
    barrier = pltpu.get_barrier_semaphore()

    def greet(d, carry):
        pl.semaphore_signal(barrier, inc=1, device_id={"bx": lax.rem(me + d, count)}, device_id_type=MESH)
        return carry

    lax.fori_loop(1, count, greet, 0)


def plan_blocks(block_len):
    windows = ((NEAR, -HALF, 5 * LANES), (FAR, -LANES, 0), (FAR, 0, LANES),
               (EDGE, -LANES - HALF, 4 * LANES), (EDGE, HALF, 6 * LANES))
    left = list(range(block_len // ROWS))
    runs = []
    for phase, column, lane in windows:
        fits = [b for b in left if column <= b * ROWS - REACH and b * ROWS + ROWS + REACH <= column + SPAN]
        left = [b for b in left if b not in fits]
        runs.append((phase, len(fits), fits[0], column, lane))
        assert fits == list(range(fits[0], fits[0] + len(fits)))
    assert not left and block_len == 2 * LANES
    return runs


def pick(value, runs):
    result = runs[-1][1]
    for bound, entry in runs[-2::-1]:
        result = jnp.where(value < bound, entry, result)
    return result


def fourfold(body):
    def step(i, carry):
        for k in range(4):
            carry = body(4 * i + k, carry)
        return carry
    return step


def features_kernel(count, bold_hbm, idx_hbm, subject_hbm, out_ref,
                    sorted_ref, win_ref, quarter_ref, halo_ref, own_ref, lane_ref, tile_ref, valid_ref,
                    sid_ref, perm_ref, x0_ref, x1_ref, sum0_ref, sum1_ref, sq0_ref, sq1_ref,
                    mean0_ref, mean1_ref, scale0_ref, scale1_ref, square_ref, total_ref, prod_ref,
                    bold_ref, idx_ref, subject_ref, load_sem, took_ref, send0, recv0, send1, recv1, send2, recv2):
    points, epochs, block_len = bold_ref.shape
    slots = idx_ref.shape[0]
    groups = epochs // GROUP
    depth = points * GROUP
    packed = points * epochs // 2
    me = lax.axis_index("bx")
    runs = plan_blocks(block_len)
    ends = [sum(r[1] for r in runs[:i + 1]) for i in range(len(runs))]

    loads = [pltpu.make_async_copy(src, dst, load_sem.at[i]) for i, (src, dst) in enumerate(
        ((subject_hbm, subject_ref), (bold_hbm, bold_ref), (idx_hbm, idx_ref)))]
    for load in loads:
        load.start()
    greet_bx(count)
    loads[0].wait()
    named = jnp.broadcast_to(subject_ref[...], (epochs, LANES))
    named_t = named.T
    row = lax.broadcasted_iota(jnp.int32, (epochs, LANES), 0)
    col = lax.broadcasted_iota(jnp.int32, (epochs, LANES), 1)
    ahead = (named_t < named) | ((named_t == named) & (row < col))
    rank = jnp.sum(ahead.astype(jnp.float32), axis=0, keepdims=True).astype(jnp.int32)
    perm = (jnp.broadcast_to(rank, (epochs, LANES)) == row).astype(jnp.float32)
    perm_ref[...] = perm
    perm16 = perm.astype(jnp.bfloat16)

    loads[1].wait()

    def arrange(t, carry):
        sorted_ref[t] = jnp.dot(perm16, bold_ref[t], preferred_element_type=jnp.float32)
        return carry

    lax.fori_loop(0, points // 4, fourfold(arrange), 0)

    blank = jnp.zeros((LANES - depth, block_len), jnp.float32)

    def tile_of(i):
        return slice(i * LANES, (i + 1) * LANES)

    def join(low, high):
        return jnp.concatenate([low, high], axis=1)

    def turned(values):
        return join(values[:, HALF:], values[:, :HALF])

    def fill(g, carry):
        cells = normalized(sorted_ref[:, pl.ds(pl.multiple_of(g * GROUP, GROUP), GROUP), :])
        cells = cells.reshape(depth, block_len).astype(jnp.bfloat16)
        rows = pl.ds(pl.multiple_of(g * depth, depth), depth)
        here0, here1 = cells[:, :LANES], cells[:, LANES:]
        turn0, turn1 = turned(here0), turned(here1)
        win_ref[rows, tile_of(1)] = here0
        win_ref[rows, tile_of(2)] = here1
        win_ref[rows, tile_of(5)] = turn0
        win_ref[rows, tile_of(6)] = join(turn0[:, :HALF], turn1[:, HALF:])
        win_ref[rows, tile_of(7)] = turn1
        return carry

    lax.fori_loop(0, groups // 4, fourfold(fill), 0)

    def pair_rows(g):
        first = pl.multiple_of(g * depth, depth)
        return pl.ds(first, depth), pl.ds(pl.multiple_of(first + packed, depth), depth)

    def pack(quarters):
        def body(g, carry):
            upper, lower = pair_rows(g)
            for q in quarters:
                one, two = ((1, 5), (5, 1), (2, 7), (7, 2))[q]
                quarter_ref[q, upper, :] = join(
                    win_ref[upper, tile_of(one)][:, :HALF], win_ref[lower, tile_of(two)][:, HALF:])
            return carry

        lax.fori_loop(0, groups // 8, fourfold(body), 0)

    pack((0, 3))
    pl.semaphore_wait(pltpu.get_barrier_semaphore(), count - 1)

    def message(side, phase):
        quarter = (3 - phase) if side == 0 else phase
        to = me + 1 if side == 0 else me - 1
        return pltpu.make_async_remote_copy(
            src_ref=quarter_ref.at[quarter], dst_ref=halo_ref.at[side * 3 + phase],
            send_sem=send0.at[side * 3 + phase], recv_sem=recv0.at[side * 3 + phase],
            device_id={"bx": to}, device_id_type=MESH)

    sends = (me < count - 1, me > 0)
    gets = (me > 0, me < count - 1)
    def send(phase):
        for side in range(2):
            @pl.when(sends[side])
            def _():
                message(side, phase).start()

    send(NEAR)
    pack((1, 2))

    for side in range(2):
        @pl.when(jnp.logical_not(gets[side]))
        def _():
            for phase in range(3):
                halo_ref[side * 3 + phase] = jnp.zeros((packed, LANES), jnp.bfloat16)

    one_row = subject_ref[...]
    starts = [jnp.clip(jnp.sum((one_row < s).astype(jnp.float32)).astype(jnp.int32), 0, epochs)
              for s in range(SUBJ + 1)]
    sid = jnp.zeros((epochs, LANES), jnp.int32)
    for s in range(1, SUBJ):
        sid = sid + (row >= starts[s]).astype(jnp.int32)
    sid_ref[...] = sid

    def turn_own(g, carry):
        rows = pl.ds(pl.multiple_of(g * depth, depth), depth)
        own = win_ref[rows, LANES:LANES + block_len].astype(jnp.float32)
        flat = jnp.concatenate([own, blank], axis=0).T
        for b in range(block_len // ROWS):
            piece = flat[b * ROWS:(b + 1) * ROWS, :]
            own_ref[b, g] = jnp.concatenate([piece, piece], axis=0).astype(jnp.bfloat16)
        return carry

    lax.fori_loop(0, groups // 4, fourfold(turn_own), 0)

    loads[2].wait()
    for half in range(block_len // LANES):
        at = idx_ref[:, half * LANES:(half + 1) * LANES].T
        centre = lax.broadcasted_iota(jnp.int32, (LANES, slots), 0) + half * LANES
        column = pick(centre // ROWS, sorted((r[2] + r[1], r[3]) for r in runs))
        offset = at - block_len - column
        part = slice(half * LANES, (half + 1) * LANES)
        valid_ref[part, :] = (at >= 0).astype(jnp.float32)
        lane_ref[part, :] = jnp.where(at >= 0, offset & (LANES - 1), 0)
        tile_ref[part, :] = jnp.where(at >= 0, offset >> 7, 0)

    def arrived(phase):
        for side in range(2):
            @pl.when(gets[side])
            def _():
                message(side, phase).wait_recv()

    def settle(phase):
        arrived(phase)
        if phase != EDGE:
            send(phase + 1)
        left, right = halo_ref.at[phase], halo_ref.at[3 + phase]
        inner_left, inner_right = (halo_ref.at[phase - 1], halo_ref.at[2 + phase]) if phase else (None, None)

        def body(g, carry):
            upper, lower = pair_rows(g)
            near_l, near_r = left[upper, :], right[upper, :]
            if phase == NEAR:
                for rows, (l, r) in ((upper, (near_l, near_r[:, :HALF])), (lower, (near_l[:, HALF:], near_r[:, HALF:]))):
                    win_ref[rows, tile_of(5)] = join(l[:, :HALF], win_ref[rows, tile_of(5)][:, HALF:])
                    win_ref[rows, tile_of(7)] = join(win_ref[rows, tile_of(7)][:, :HALF], r)
            else:
                in_l, in_r = inner_left[upper, :], inner_right[upper, :]
                a, b = (0, 3) if phase == FAR else (4, 8)
                for rows, cut in ((upper, slice(0, HALF)), (lower, slice(HALF, LANES))):
                    win_ref[rows, tile_of(a)] = join(near_l[:, cut], in_l[:, cut])
                    win_ref[rows, tile_of(b)] = join(in_r[:, cut], near_r[:, cut])
            return carry

        lax.fori_loop(0, groups // 8, fourfold(body), 0)

    total_ref[...] = jnp.zeros_like(total_ref)
    masks = []
    for p in range(GROUP // 2):
        which = lax.broadcasted_iota(jnp.int32, (2 * ROWS, LANES), 0) // ROWS + 2 * p
        lane = lax.broadcasted_iota(jnp.int32, (2 * ROWS, LANES), 1) % GROUP
        masks.append((which == lane).astype(jnp.float32).astype(jnp.bfloat16))
    inverse = [1.0 / jnp.maximum((starts[s + 1] - starts[s]).astype(jnp.float32), 1.0) for s in range(SUBJ)]
    for sum_ref, sq_ref in ((sum0_ref, sq0_ref), (sum1_ref, sq1_ref)):
        sum_ref[0] = jnp.zeros((ROWS, LANES), jnp.float32)
        sq_ref[0] = jnp.zeros((ROWS, LANES), jnp.float32)

    def nth(n):
        n = jnp.asarray(n, jnp.int32)
        block = n + pick(n, [(end, r[2] - (end - r[1])) for end, r in zip(ends, runs)])
        lane = pick(n, [(end, r[4]) for end, r in zip(ends, runs)])
        return block, pl.multiple_of(lane, LANES)

    def product(at, g):
        b, start = at
        rhs = win_ref[g * depth:(g + 1) * depth, pl.ds(start, SPAN)]
        own = own_ref[b, g]
        lhs = jnp.concatenate([own * m for m in masks], axis=0)[:, :depth]
        return jnp.dot(lhs, rhs, preferred_element_type=jnp.float32)

    def correlate(at, refs, queue, after):
        b = at[0]
        x_ref, sum_ref, sq_ref = refs[:3]
        here = pl.ds(pl.multiple_of(b * ROWS, ROWS), ROWS)
        lane = lane_ref[here, :]
        tile = tile_ref[here, :]
        first = tile == 0
        second = tile == 1
        running = jnp.zeros((ROWS, LANES), jnp.float32)
        squares = jnp.zeros((ROWS, LANES), jnp.float32)
        for g in range(groups):
            prod = queue.pop(0)
            for e in range(GROUP):
                r = e * ROWS
                parts = [take(prod[r:r + ROWS, t * LANES:(t + 1) * LANES], lane, BY_LANE)
                         for t in range(SPAN // LANES)]
                x = jnp.where(first, parts[0], jnp.where(second, parts[1], parts[2]))
                i = g * GROUP + e
                x_ref[i * ROWS:(i + 1) * ROWS, :] = x
                running = running + x
                squares = squares + x * x
                sum_ref[i + 1] = running
                sq_ref[i + 1] = squares
            ahead = g + AHEAD
            if ahead < groups:
                queue.append(product(at, ahead))
            elif after is not None:
                queue.append(product(after, ahead - groups))
            yield

    def kernels(b, refs):
        x_ref, sum_ref, sq_ref, mean_ref, scale_ref = refs
        valid = valid_ref[pl.ds(pl.multiple_of(b * ROWS, ROWS), ROWS), :]
        for s in range(SUBJ):
            mean = (sum_ref[starts[s + 1]] - sum_ref[starts[s]]) * inverse[s]
            second = (sq_ref[starts[s + 1]] - sq_ref[starts[s]]) * inverse[s]
            var = jnp.maximum(second - mean * mean, 0.0)
            mean_ref[s * ROWS:(s + 1) * ROWS, :] = mean
            scale_ref[s * ROWS:(s + 1) * ROWS, :] = lax.rsqrt(var + VARIANCE_FLOOR) * valid
        acc = None
        for r in range(ROWS):
            mean = mean_ref[pl.ds(r, SUBJ, stride=ROWS), :]
            scale = scale_ref[pl.ds(r, SUBJ, stride=ROWS), :]
            pieces = []
            for q in range(epochs // 8):
                at = sid_ref[q * 8:(q + 1) * 8, :]
                x = x_ref[pl.ds(q * 8 * ROWS + r, 8, stride=ROWS), :]
                pieces.append((x - take(mean, at, BY_ROW)) * take(scale, at, BY_ROW))
            feat = jnp.concatenate(pieces, axis=0).astype(jnp.bfloat16)
            kern = lax.dot_general(feat, feat, (((1,), (1,)), ((), ())), preferred_element_type=jnp.float32)
            part = jnp.sum((kern * kern).reshape(epochs // 8, 8, epochs), axis=0)
            square_ref[pl.ds(pl.multiple_of((b * ROWS + r) * 8, 8), 8), :] = part
            acc = kern if acc is None else acc + kern
            yield
        total_ref[...] += acc

    even = (x0_ref, sum0_ref, sq0_ref, mean0_ref, scale0_ref)
    odd = (x1_ref, sum1_ref, sq1_ref, mean1_ref, scale1_ref)
    blocks = block_len // ROWS

    def together(first, second):
        pace = groups // ROWS
        for _ in range(ROWS):
            for _ in range(pace):
                next(first)
            next(second)
        for rest in (first, second):
            for _ in rest:
                pass

    def keep(queue):
        for i, prod in enumerate(queue):
            prod_ref[i] = prod

    settle(NEAR)
    queue = [product(nth(0), g) for g in range(AHEAD)]
    for _ in correlate(nth(0), even, queue, nth(1)):
        pass
    keep(queue)
    near = sum(r[1] for r in runs if r[0] == NEAR)
    outer = sum(r[1] for r in runs if r[0] == EDGE)

    def two_blocks(j, carry):
        n = 2 * j

        @pl.when(j == (near - 3) // 2 + 1)
        def _():
            settle(FAR)

        @pl.when(j == (blocks - outer - 3) // 2 + 1)
        def _():
            settle(EDGE)

        queue = [prod_ref[i] for i in range(AHEAD)]
        last = nth(n + 2)
        together(correlate(nth(n + 1), odd, queue, last), kernels(nth(n)[0], even))
        together(correlate(last, even, queue, nth(n + 3)), kernels(nth(n + 1)[0], odd))
        keep(queue)
        return carry

    lax.fori_loop(0, blocks // 2 - 1, two_blocks, 0)
    queue = [prod_ref[i] for i in range(AHEAD)]
    together(correlate(nth(blocks - 1), odd, queue, None), kernels(nth(blocks - 2)[0], even))
    for _ in kernels(nth(blocks - 1)[0], odd):
        pass

    exact = lax.Precision.HIGHEST
    half_way = jnp.dot(total_ref[...], perm_ref[...], precision=exact, preferred_element_type=jnp.float32)
    total_ref[...] = jnp.dot(perm_ref[...].T, half_way, precision=exact, preferred_element_type=jnp.float32)
    for phase in range(3):
        for side in range(2):
            @pl.when(sends[side])
            def _():
                message(side, phase).wait_send()

    def spreads():
        for half in range(block_len // LANES):
            sums = None
            for r in range(8):
                part = square_ref[pl.ds(half * LANES * 8 + r, LANES, stride=8), :]
                sums = part if sums is None else sums + part
            sums = jnp.sum(sums.T, axis=0, keepdims=True)
            out_ref[epochs + half:epochs + half + 1, :] = jnp.sqrt(sums * (1.0 / (epochs * NB * NB)))

    reduce_over_bx(count, 1.0 / (NB * block_len * count), spreads, total_ref, out_ref, took_ref, send1, recv1, send2, recv2)


def per_device(bold, nbr_table, subject):
    epochs, points, block_len = bold.shape
    slots = nbr_table.shape[0]
    count = lax.axis_size("bx")
    bold = bold.transpose(1, 0, 2)
    vmem = pl.BlockSpec(memory_space=pltpu.VMEM)
    groups = epochs // GROUP
    f32 = functools.partial(pltpu.VMEM, dtype=jnp.float32)
    packed = pl.pallas_call(
        functools.partial(features_kernel, count),
        in_specs=[pl.BlockSpec(memory_space=pl.ANY)] * 3,
        out_specs=vmem,
        out_shape=jax.ShapeDtypeStruct((epochs + ROWS, epochs), jnp.float32),
        scratch_shapes=[
            f32((points, epochs, block_len)),
            pltpu.VMEM((points * epochs, 9 * LANES), jnp.bfloat16),
            pltpu.VMEM((4, points * epochs // 2, LANES), jnp.bfloat16),
            pltpu.VMEM((6, points * epochs // 2, LANES), jnp.bfloat16),
            pltpu.VMEM((block_len // ROWS, groups, 2 * ROWS, LANES), jnp.bfloat16),
            pltpu.VMEM((block_len, slots), jnp.int32),
            pltpu.VMEM((block_len, slots), jnp.int32),
            f32((block_len, slots)),
            pltpu.VMEM((epochs, LANES), jnp.int32),
            f32((epochs, epochs)),
            *[f32((epochs * ROWS, LANES))] * 2,
            *[f32((epochs + 1, ROWS, LANES))] * 4,
            *[f32((SUBJ * ROWS, LANES))] * 4,
            f32((block_len * 8, epochs)),
            f32((epochs, epochs)),
            f32((AHEAD, GROUP * ROWS, SPAN)),
            pltpu.VMEM((points, epochs, block_len), jnp.bfloat16),
            pltpu.VMEM((slots, block_len), jnp.int32),
            pltpu.VMEM((1, epochs), jnp.int32),
            pltpu.SemaphoreType.DMA((3,)),
            f32((count, epochs // count, epochs)),
            *[pltpu.SemaphoreType.DMA((6,))] * 2,
            *[pltpu.SemaphoreType.DMA((count,))] * 4,
        ],
        compiler_params=pltpu.CompilerParams(collective_id=0, has_side_effects=True,
                                             vmem_limit_bytes=60 * 1024 * 1024),
        name="features",
    )(bold, nbr_table, subject[None, :])
    spread = packed[epochs:epochs + block_len // LANES].reshape(block_len)
    return spread, packed[:epochs]


def solution(mesh):
    return jax.shard_map(
        per_device,
        mesh=mesh,
        in_specs=(P("cohort", None, "bx"), P("cohort", "bx"), P("cohort")),
        out_specs=(P(("cohort", "bx")), P("cohort", None)),
        check_vma=False,
    )
```

```python
import functools

import jax
import jax.numpy as jnp
from jax import lax
from jax.experimental import pallas as pl
from jax.experimental.pallas import tpu as pltpu
from jax.sharding import PartitionSpec as P

NB = 125
SUBJ = 8
REACH = 147
VARIANCE_FLOOR = 0.05

LANES = 128
ROWS = 8
GROUP = 8
AHEAD = 5
HALF = 64
SPAN = 384
NEAR, FAR, EDGE = range(3)
MESH = pl.DeviceIdType.MESH
BY_ROW = lax.GatherDimensionNumbers(
    offset_dims=(), collapsed_slice_dims=(0,), start_index_map=(0,),
    operand_batching_dims=(1,), start_indices_batching_dims=(1,))
BY_LANE = lax.GatherDimensionNumbers(
    offset_dims=(), collapsed_slice_dims=(1,), start_index_map=(1,),
    operand_batching_dims=(0,), start_indices_batching_dims=(0,))


def take(values, at, dims):
    return lax.gather(values, at[..., None], dims, (1, 1), mode="promise_in_bounds")


def normalized(values):
    points = values.shape[0]
    centred = values - jnp.sum(values, axis=0, keepdims=True) * (1.0 / points)
    return centred * (1.0 / jnp.sqrt(jnp.sum(centred * centred, axis=0, keepdims=True) + 1.0))


def owners_of(count):
    owners = max(count // 2, 1)
    return owners, (count - owners) // 2


def reduce_over_bx(count, scale, between, part_ref, out_ref, took, send1, recv1, send2, recv2):
    me = lax.axis_index("bx")
    owners, first = owners_of(count)
    rows = part_ref.shape[0] // owners
    mine = me - first
    owner = (mine >= 0) & (mine < owners)

    def block(i):
        return pl.ds(pl.multiple_of(i * rows, rows), rows)

    def scatter(k, source):
        return pltpu.make_async_remote_copy(
            src_ref=part_ref.at[block(k)], dst_ref=took.at[source], send_sem=send1.at[k], recv_sem=recv1.at[source],
            device_id={"bx": first + k}, device_id_type=MESH)

    def gather(k, d):
        return pltpu.make_async_remote_copy(
            src_ref=out_ref.at[block(k)], dst_ref=out_ref.at[block(k)], send_sem=send2.at[d], recv_sem=recv2.at[k],
            device_id={"bx": lax.rem(me + d, count)}, device_id_type=MESH)

    def each(low, high, skip, act):
        def body(i, carry):
            @pl.when(i != skip)
            def _():
                act(i)
            return carry
        if count <= 16:
            for i in range(low, high):
                body(i, 0)
        else:
            lax.fori_loop(low, high, body, 0)

    each(0, owners, mine, lambda k: scatter(k, me).start())
    between()

    @pl.when(owner)
    def _():
        took[me] = part_ref[block(mine), :]
        each(0, count, me, lambda source: scatter(mine, source).wait_recv())
        out_ref[block(mine), :] = lax.fori_loop(1, count, lambda i, total: total + took[i], took[0]) * scale
        each(1, count, 0, lambda d: gather(mine, d).start())

    each(0, owners, mine, lambda k: scatter(k, me).wait_send())
    each(0, owners, mine, lambda k: gather(k, 0).wait_recv())

    @pl.when(owner)
    def _():
        each(1, count, 0, lambda d: gather(mine, d).wait_send())


def greet_bx(count):
    me = lax.axis_index("bx")
    barrier = pltpu.get_barrier_semaphore()

    def greet(d, carry):
        pl.semaphore_signal(barrier, inc=1, device_id={"bx": lax.rem(me + d, count)}, device_id_type=MESH)
        return carry

    lax.fori_loop(1, count, greet, 0)


def plan_blocks(block_len):
    windows = ((NEAR, -HALF, 5 * LANES), (FAR, -LANES, 0), (FAR, 0, LANES),
               (EDGE, -LANES - HALF, 4 * LANES), (EDGE, HALF, 6 * LANES))
    left = list(range(block_len // ROWS))
    runs = []
    for phase, column, lane in windows:
        fits = [b for b in left if column <= b * ROWS - REACH and b * ROWS + ROWS + REACH <= column + SPAN]
        left = [b for b in left if b not in fits]
        runs.append((phase, len(fits), fits[0], column, lane))
        assert fits == list(range(fits[0], fits[0] + len(fits)))
    assert not left and block_len == 2 * LANES
    return runs


def pick(value, runs):
    result = runs[-1][1]
    for bound, entry in runs[-2::-1]:
        result = jnp.where(value < bound, entry, result)
    return result


def fourfold(body):
    def step(i, carry):
        for k in range(4):
            carry = body(4 * i + k, carry)
        return carry
    return step


def features_kernel(count, bold_hbm, idx_hbm, subject_hbm, out_ref,
                    sorted_ref, win_ref, quarter_ref, halo_ref, own_ref, lane_ref, tile_ref, valid_ref,
                    sid_ref, perm_ref, x0_ref, x1_ref, sum0_ref, sum1_ref, sq0_ref, sq1_ref,
                    mean0_ref, mean1_ref, scale0_ref, scale1_ref, square_ref, total_ref, prod_ref,
                    bold_ref, idx_ref, subject_ref, load_sem, took_ref, send0, recv0, send1, recv1, send2, recv2):
    points, epochs, block_len = bold_ref.shape
    slots = idx_ref.shape[0]
    groups = epochs // GROUP
    depth = points * GROUP
    packed = points * epochs // 2
    me = lax.axis_index("bx")
    runs = plan_blocks(block_len)
    ends = [sum(r[1] for r in runs[:i + 1]) for i in range(len(runs))]

    loads = [pltpu.make_async_copy(src, dst, load_sem.at[i]) for i, (src, dst) in enumerate(
        ((subject_hbm, subject_ref), (bold_hbm, bold_ref), (idx_hbm, idx_ref)))]
    for load in loads:
        load.start()
    greet_bx(count)
    loads[0].wait()
    named = jnp.broadcast_to(subject_ref[...], (epochs, LANES))
    named_t = named.T
    row = lax.broadcasted_iota(jnp.int32, (epochs, LANES), 0)
    col = lax.broadcasted_iota(jnp.int32, (epochs, LANES), 1)
    ahead = (named_t < named) | ((named_t == named) & (row < col))
    rank = jnp.sum(ahead.astype(jnp.float32), axis=0, keepdims=True).astype(jnp.int32)
    perm = (jnp.broadcast_to(rank, (epochs, LANES)) == row).astype(jnp.float32)
    perm_ref[...] = perm
    perm16 = perm.astype(jnp.bfloat16)

    loads[1].wait()

    def arrange(t, carry):
        sorted_ref[t] = jnp.dot(perm16, bold_ref[t], preferred_element_type=jnp.float32)
        return carry

    lax.fori_loop(0, points // 4, fourfold(arrange), 0)

    blank = jnp.zeros((LANES - depth, block_len), jnp.float32)

    def tile_of(i):
        return slice(i * LANES, (i + 1) * LANES)

    def join(low, high):
        return jnp.concatenate([low, high], axis=1)

    def turned(values):
        return join(values[:, HALF:], values[:, :HALF])

    def fill(g, carry):
        cells = normalized(sorted_ref[:, pl.ds(pl.multiple_of(g * GROUP, GROUP), GROUP), :])
        cells = cells.reshape(depth, block_len).astype(jnp.bfloat16)
        rows = pl.ds(pl.multiple_of(g * depth, depth), depth)
        here0, here1 = cells[:, :LANES], cells[:, LANES:]
        turn0, turn1 = turned(here0), turned(here1)
        win_ref[rows, tile_of(1)] = here0
        win_ref[rows, tile_of(2)] = here1
        win_ref[rows, tile_of(5)] = turn0
        win_ref[rows, tile_of(6)] = join(turn0[:, :HALF], turn1[:, HALF:])
        win_ref[rows, tile_of(7)] = turn1
        return carry

    lax.fori_loop(0, groups // 4, fourfold(fill), 0)

    def pair_rows(g):
        first = pl.multiple_of(g * depth, depth)
        return pl.ds(first, depth), pl.ds(pl.multiple_of(first + packed, depth), depth)

    def pack(quarters):
        def body(g, carry):
            upper, lower = pair_rows(g)
            for q in quarters:
                one, two = ((1, 5), (5, 1), (2, 7), (7, 2))[q]
                quarter_ref[q, upper, :] = join(
                    win_ref[upper, tile_of(one)][:, :HALF], win_ref[lower, tile_of(two)][:, HALF:])
            return carry

        lax.fori_loop(0, groups // 8, fourfold(body), 0)

    pack((0, 3))
    pl.semaphore_wait(pltpu.get_barrier_semaphore(), count - 1)

    def message(side, phase):
        quarter = (3 - phase) if side == 0 else phase
        to = me + 1 if side == 0 else me - 1
        return pltpu.make_async_remote_copy(
            src_ref=quarter_ref.at[quarter], dst_ref=halo_ref.at[side * 3 + phase],
            send_sem=send0.at[side * 3 + phase], recv_sem=recv0.at[side * 3 + phase],
            device_id={"bx": to}, device_id_type=MESH)

    sends = (me < count - 1, me > 0)
    gets = (me > 0, me < count - 1)
    def send(phase):
        for side in range(2):
            @pl.when(sends[side])
            def _():
                message(side, phase).start()

    send(NEAR)
    pack((1, 2))

    for side in range(2):
        @pl.when(jnp.logical_not(gets[side]))
        def _():
            for phase in range(3):
                halo_ref[side * 3 + phase] = jnp.zeros((packed, LANES), jnp.bfloat16)

    one_row = subject_ref[...]
    starts = [jnp.clip(jnp.sum((one_row < s).astype(jnp.float32)).astype(jnp.int32), 0, epochs)
              for s in range(SUBJ + 1)]
    sid = jnp.zeros((epochs, LANES), jnp.int32)
    for s in range(1, SUBJ):
        sid = sid + (row >= starts[s]).astype(jnp.int32)
    sid_ref[...] = sid

    def turn_own(g, carry):
        rows = pl.ds(pl.multiple_of(g * depth, depth), depth)
        own = win_ref[rows, LANES:LANES + block_len].astype(jnp.float32)
        flat = jnp.concatenate([own, blank], axis=0).T
        for b in range(block_len // ROWS):
            piece = flat[b * ROWS:(b + 1) * ROWS, :]
            own_ref[b, g] = jnp.concatenate([piece, piece], axis=0).astype(jnp.bfloat16)
        return carry

    lax.fori_loop(0, groups // 4, fourfold(turn_own), 0)

    loads[2].wait()
    for half in range(block_len // LANES):
        at = idx_ref[:, half * LANES:(half + 1) * LANES].T
        centre = lax.broadcasted_iota(jnp.int32, (LANES, slots), 0) + half * LANES
        column = pick(centre // ROWS, sorted((r[2] + r[1], r[3]) for r in runs))
        offset = at - block_len - column
        part = slice(half * LANES, (half + 1) * LANES)
        valid_ref[part, :] = (at >= 0).astype(jnp.float32)
        lane_ref[part, :] = jnp.where(at >= 0, offset & (LANES - 1), 0)
        tile_ref[part, :] = jnp.where(at >= 0, offset >> 7, 0)

    def arrived(phase):
        for side in range(2):
            @pl.when(gets[side])
            def _():
                message(side, phase).wait_recv()

    def settle(phase):
        arrived(phase)
        if phase != EDGE:
            send(phase + 1)
        left, right = halo_ref.at[phase], halo_ref.at[3 + phase]
        inner_left, inner_right = (halo_ref.at[phase - 1], halo_ref.at[2 + phase]) if phase else (None, None)

        def body(g, carry):
            upper, lower = pair_rows(g)
            near_l, near_r = left[upper, :], right[upper, :]
            if phase == NEAR:
                for rows, (l, r) in ((upper, (near_l, near_r[:, :HALF])), (lower, (near_l[:, HALF:], near_r[:, HALF:]))):
                    win_ref[rows, tile_of(5)] = join(l[:, :HALF], win_ref[rows, tile_of(5)][:, HALF:])
                    win_ref[rows, tile_of(7)] = join(win_ref[rows, tile_of(7)][:, :HALF], r)
            else:
                in_l, in_r = inner_left[upper, :], inner_right[upper, :]
                a, b = (0, 3) if phase == FAR else (4, 8)
                for rows, cut in ((upper, slice(0, HALF)), (lower, slice(HALF, LANES))):
                    win_ref[rows, tile_of(a)] = join(near_l[:, cut], in_l[:, cut])
                    win_ref[rows, tile_of(b)] = join(in_r[:, cut], near_r[:, cut])
            return carry

        lax.fori_loop(0, groups // 8, fourfold(body), 0)

    total_ref[...] = jnp.zeros_like(total_ref)
    masks = []
    for p in range(GROUP // 2):
        which = lax.broadcasted_iota(jnp.int32, (2 * ROWS, LANES), 0) // ROWS + 2 * p
        lane = lax.broadcasted_iota(jnp.int32, (2 * ROWS, LANES), 1) % GROUP
        masks.append((which == lane).astype(jnp.float32).astype(jnp.bfloat16))
    inverse = [1.0 / jnp.maximum((starts[s + 1] - starts[s]).astype(jnp.float32), 1.0) for s in range(SUBJ)]
    for sum_ref, sq_ref in ((sum0_ref, sq0_ref), (sum1_ref, sq1_ref)):
        sum_ref[0] = jnp.zeros((ROWS, LANES), jnp.float32)
        sq_ref[0] = jnp.zeros((ROWS, LANES), jnp.float32)

    def nth(n):
        n = jnp.asarray(n, jnp.int32)
        block = n + pick(n, [(end, r[2] - (end - r[1])) for end, r in zip(ends, runs)])
        lane = pick(n, [(end, r[4]) for end, r in zip(ends, runs)])
        return block, pl.multiple_of(lane, LANES)

    def product(at, g):
        b, start = at
        rhs = win_ref[g * depth:(g + 1) * depth, pl.ds(start, SPAN)]
        own = own_ref[b, g]
        lhs = jnp.concatenate([own * m for m in masks], axis=0)[:, :depth]
        return jnp.dot(lhs, rhs, preferred_element_type=jnp.float32)

    def correlate(at, refs, queue, after):
        b = at[0]
        x_ref, sum_ref, sq_ref = refs[:3]
        here = pl.ds(pl.multiple_of(b * ROWS, ROWS), ROWS)
        lane = lane_ref[here, :]
        tile = tile_ref[here, :]
        first = tile == 0
        second = tile == 1
        running = jnp.zeros((ROWS, LANES), jnp.float32)
        squares = jnp.zeros((ROWS, LANES), jnp.float32)
        for g in range(groups):
            prod = queue.pop(0)
            for e in range(GROUP):
                r = e * ROWS
                parts = [take(prod[r:r + ROWS, t * LANES:(t + 1) * LANES], lane, BY_LANE)
                         for t in range(SPAN // LANES)]
                x = jnp.where(first, parts[0], jnp.where(second, parts[1], parts[2]))
                i = g * GROUP + e
                x_ref[i * ROWS:(i + 1) * ROWS, :] = x
                running = running + x
                squares = squares + x * x
                sum_ref[i + 1] = running
                sq_ref[i + 1] = squares
            ahead = g + AHEAD
            if ahead < groups:
                queue.append(product(at, ahead))
            elif after is not None:
                queue.append(product(after, ahead - groups))
            yield

    def kernels(b, refs):
        x_ref, sum_ref, sq_ref, mean_ref, scale_ref = refs
        valid = valid_ref[pl.ds(pl.multiple_of(b * ROWS, ROWS), ROWS), :]
        for s in range(SUBJ):
            mean = (sum_ref[starts[s + 1]] - sum_ref[starts[s]]) * inverse[s]
            second = (sq_ref[starts[s + 1]] - sq_ref[starts[s]]) * inverse[s]
            var = jnp.maximum(second - mean * mean, 0.0)
            mean_ref[s * ROWS:(s + 1) * ROWS, :] = mean
            scale_ref[s * ROWS:(s + 1) * ROWS, :] = lax.rsqrt(var + VARIANCE_FLOOR) * valid
        acc = None
        for r in range(ROWS):
            mean = mean_ref[pl.ds(r, SUBJ, stride=ROWS), :]
            scale = scale_ref[pl.ds(r, SUBJ, stride=ROWS), :]
            pieces = []
            for q in range(epochs // 8):
                at = sid_ref[q * 8:(q + 1) * 8, :]
                x = x_ref[pl.ds(q * 8 * ROWS + r, 8, stride=ROWS), :]
                pieces.append((x - take(mean, at, BY_ROW)) * take(scale, at, BY_ROW))
            feat = jnp.concatenate(pieces, axis=0).astype(jnp.bfloat16)
            kern = lax.dot_general(feat, feat, (((1,), (1,)), ((), ())), preferred_element_type=jnp.float32)
            part = jnp.sum((kern * kern).reshape(epochs // 8, 8, epochs), axis=0)
            square_ref[pl.ds(pl.multiple_of((b * ROWS + r) * 8, 8), 8), :] = part
            acc = kern if acc is None else acc + kern
            yield
        total_ref[...] += acc

    even = (x0_ref, sum0_ref, sq0_ref, mean0_ref, scale0_ref)
    odd = (x1_ref, sum1_ref, sq1_ref, mean1_ref, scale1_ref)
    blocks = block_len // ROWS

    def together(first, second):
        pace = groups // ROWS
        for _ in range(ROWS):
            for _ in range(pace):
                next(first)
            next(second)
        for rest in (first, second):
            for _ in rest:
                pass

    def keep(queue):
        for i, prod in enumerate(queue):
            prod_ref[i] = prod

    settle(NEAR)
    queue = [product(nth(0), g) for g in range(AHEAD)]
    for _ in correlate(nth(0), even, queue, nth(1)):
        pass
    keep(queue)
    near = sum(r[1] for r in runs if r[0] == NEAR)
    outer = sum(r[1] for r in runs if r[0] == EDGE)

    def two_blocks(j, carry):
        n = 2 * j

        @pl.when(j == (near - 3) // 2 + 1)
        def _():
            settle(FAR)

        @pl.when(j == (blocks - outer - 3) // 2 + 1)
        def _():
            settle(EDGE)

        queue = [prod_ref[i] for i in range(AHEAD)]
        last = nth(n + 2)
        together(correlate(nth(n + 1), odd, queue, last), kernels(nth(n)[0], even))
        together(correlate(last, even, queue, nth(n + 3)), kernels(nth(n + 1)[0], odd))
        keep(queue)
        return carry

    lax.fori_loop(0, blocks // 2 - 1, two_blocks, 0)
    queue = [prod_ref[i] for i in range(AHEAD)]
    together(correlate(nth(blocks - 1), odd, queue, None), kernels(nth(blocks - 2)[0], even))
    for _ in kernels(nth(blocks - 1)[0], odd):
        pass

    exact = lax.Precision.HIGHEST
    half_way = jnp.dot(total_ref[...], perm_ref[...], precision=exact, preferred_element_type=jnp.float32)
    total_ref[...] = jnp.dot(perm_ref[...].T, half_way, precision=exact, preferred_element_type=jnp.float32)
    for phase in range(3):
        for side in range(2):
            @pl.when(sends[side])
            def _():
                message(side, phase).wait_send()

    def spreads():
        for half in range(block_len // LANES):
            sums = None
            for r in range(8):
                part = square_ref[pl.ds(half * LANES * 8 + r, LANES, stride=8), :]
                sums = part if sums is None else sums + part
            sums = jnp.sum(sums.T, axis=0, keepdims=True)
            out_ref[epochs + half:epochs + half + 1, :] = jnp.sqrt(sums * (1.0 / (epochs * NB * NB)))

    reduce_over_bx(count, 1.0 / (NB * block_len * count), spreads, total_ref, out_ref, took_ref, send1, recv1, send2, recv2)


def per_device(bold, nbr_table, subject):
    epochs, points, block_len = bold.shape
    slots = nbr_table.shape[0]
    count = lax.axis_size("bx")
    bold = bold.transpose(1, 0, 2)
    vmem = pl.BlockSpec(memory_space=pltpu.VMEM)
    groups = epochs // GROUP
    f32 = functools.partial(pltpu.VMEM, dtype=jnp.float32)
    packed = pl.pallas_call(
        functools.partial(features_kernel, count),
        in_specs=[pl.BlockSpec(memory_space=pl.ANY)] * 3,
        out_specs=vmem,
        out_shape=jax.ShapeDtypeStruct((epochs + ROWS, epochs), jnp.float32),
        scratch_shapes=[
            f32((points, epochs, block_len)),
            pltpu.VMEM((points * epochs, 9 * LANES), jnp.bfloat16),
            pltpu.VMEM((4, points * epochs // 2, LANES), jnp.bfloat16),
            pltpu.VMEM((6, points * epochs // 2, LANES), jnp.bfloat16),
            pltpu.VMEM((block_len // ROWS, groups, 2 * ROWS, LANES), jnp.bfloat16),
            pltpu.VMEM((block_len, slots), jnp.int32),
            pltpu.VMEM((block_len, slots), jnp.int32),
            f32((block_len, slots)),
            pltpu.VMEM((epochs, LANES), jnp.int32),
            f32((epochs, epochs)),
            *[f32((epochs * ROWS, LANES))] * 2,
            *[f32((epochs + 1, ROWS, LANES))] * 4,
            *[f32((SUBJ * ROWS, LANES))] * 4,
            f32((block_len * 8, epochs)),
            f32((epochs, epochs)),
            f32((AHEAD, GROUP * ROWS, SPAN)),
            pltpu.VMEM((points, epochs, block_len), jnp.bfloat16),
            pltpu.VMEM((slots, block_len), jnp.int32),
            pltpu.VMEM((1, epochs), jnp.int32),
            pltpu.SemaphoreType.DMA((3,)),
            f32((count, epochs // owners_of(count)[0], epochs)),
            *[pltpu.SemaphoreType.DMA((6,))] * 2,
            *[pltpu.SemaphoreType.DMA((count,))] * 4,
        ],
        compiler_params=pltpu.CompilerParams(collective_id=0, has_side_effects=True,
                                             vmem_limit_bytes=60 * 1024 * 1024),
        name="features",
    )(bold, nbr_table, subject[None, :])
    spread = packed[epochs:epochs + block_len // LANES].reshape(block_len)
    return spread, packed[:epochs]


def solution(mesh):
    return jax.shard_map(
        per_device,
        mesh=mesh,
        in_specs=(P("cohort", None, "bx"), P("cohort", "bx"), P("cohort")),
        out_specs=(P(("cohort", "bx")), P("cohort", None)),
        check_vma=False,
    )
```

```python
import functools

import jax
import jax.numpy as jnp
from jax import lax
from jax.experimental import pallas as pl
from jax.experimental.pallas import tpu as pltpu
from jax.sharding import PartitionSpec as P

NB = 125
SUBJ = 8
REACH = 147
VARIANCE_FLOOR = 0.05

LANES = 128
ROWS = 8
GROUP = 8
AHEAD = 5
HALF = 64
SPAN = 384
NEAR, FAR, EDGE = range(3)
MESH = pl.DeviceIdType.MESH
BY_ROW = lax.GatherDimensionNumbers(
    offset_dims=(), collapsed_slice_dims=(0,), start_index_map=(0,),
    operand_batching_dims=(1,), start_indices_batching_dims=(1,))
BY_LANE = lax.GatherDimensionNumbers(
    offset_dims=(), collapsed_slice_dims=(1,), start_index_map=(1,),
    operand_batching_dims=(0,), start_indices_batching_dims=(0,))


def take(values, at, dims):
    return lax.gather(values, at[..., None], dims, (1, 1), mode="promise_in_bounds")


def normalized(values):
    points = values.shape[0]
    centred = values - jnp.sum(values, axis=0, keepdims=True) * (1.0 / points)
    return centred * (1.0 / jnp.sqrt(jnp.sum(centred * centred, axis=0, keepdims=True) + 1.0))


def owners_of(count):
    owners = max(count // 2, 1)
    return owners, (count - owners) // 2


def reduce_over_bx(count, scale, between, part_ref, out_ref, took, send1, recv1, send2, recv2):
    me = lax.axis_index("bx")
    owners, first = owners_of(count)
    rows = part_ref.shape[0] // owners
    mine = me - first
    owner = (mine >= 0) & (mine < owners)

    def block(i):
        return pl.ds(pl.multiple_of(i * rows, rows), rows)

    def scatter(k, source):
        return pltpu.make_async_remote_copy(
            src_ref=part_ref.at[block(k)], dst_ref=took.at[source], send_sem=send1.at[k], recv_sem=recv1.at[source],
            device_id={"bx": first + k}, device_id_type=MESH)

    def gather(k, d):
        return pltpu.make_async_remote_copy(
            src_ref=out_ref.at[block(k)], dst_ref=out_ref.at[block(k)], send_sem=send2.at[d], recv_sem=recv2.at[k],
            device_id={"bx": lax.rem(me + d, count)}, device_id_type=MESH)

    def each(low, high, skip, act):
        def body(i, carry):
            @pl.when(i != skip)
            def _():
                act(i)
            return carry
        if count <= 16:
            for i in range(low, high):
                body(i, 0)
        else:
            lax.fori_loop(low, high, body, 0)

    each(0, owners, mine, lambda k: scatter(k, me).start())
    between()

    @pl.when(owner)
    def _():
        took[me] = part_ref[block(mine), :]
        each(0, count, me, lambda source: scatter(mine, source).wait_recv())
        out_ref[block(mine), :] = lax.fori_loop(1, count, lambda i, total: total + took[i], took[0]) * scale
        each(1, count, 0, lambda d: gather(mine, d).start())

    each(0, owners, mine, lambda k: scatter(k, me).wait_send())
    each(0, owners, mine, lambda k: gather(k, 0).wait_recv())

    @pl.when(owner)
    def _():
        each(1, count, 0, lambda d: gather(mine, d).wait_send())


def greet_bx(count):
    me = lax.axis_index("bx")
    barrier = pltpu.get_barrier_semaphore()

    def greet(d, carry):
        pl.semaphore_signal(barrier, inc=1, device_id={"bx": lax.rem(me + d, count)}, device_id_type=MESH)
        return carry

    lax.fori_loop(1, count, greet, 0)


def plan_blocks(block_len):
    windows = ((NEAR, -HALF, 5 * LANES), (FAR, -LANES, 0), (FAR, 0, LANES),
               (EDGE, -LANES - HALF, 4 * LANES), (EDGE, HALF, 6 * LANES))
    left = list(range(block_len // ROWS))
    runs = []
    for phase, column, lane in windows:
        fits = [b for b in left if column <= b * ROWS - REACH and b * ROWS + ROWS + REACH <= column + SPAN]
        left = [b for b in left if b not in fits]
        runs.append((phase, len(fits), fits[0], column, lane))
        assert fits == list(range(fits[0], fits[0] + len(fits)))
    assert not left and block_len == 2 * LANES
    return runs


def pick(value, runs):
    result = runs[-1][1]
    for bound, entry in runs[-2::-1]:
        result = jnp.where(value < bound, entry, result)
    return result


def eightfold(body):
    def step(i, carry):
        for k in range(8):
            carry = body(8 * i + k, carry)
        return carry
    return step


def fourfold(body):
    def step(i, carry):
        for k in range(4):
            carry = body(4 * i + k, carry)
        return carry
    return step


def features_kernel(count, bold_hbm, idx_hbm, subject_hbm, out_ref,
                    sorted_ref, win_ref, quarter_ref, halo_ref, own_ref, lane_ref, tile_ref, valid_ref,
                    sid_ref, perm_ref, x0_ref, x1_ref, sum0_ref, sum1_ref, sq0_ref, sq1_ref,
                    mean0_ref, mean1_ref, scale0_ref, scale1_ref, square_ref, total_ref, prod_ref,
                    bold_ref, idx_ref, subject_ref, load_sem, took_ref, send0, recv0, send1, recv1, send2, recv2):
    points, epochs, block_len = bold_ref.shape
    slots = idx_ref.shape[0]
    groups = epochs // GROUP
    depth = points * GROUP
    packed = points * epochs // 2
    me = lax.axis_index("bx")
    runs = plan_blocks(block_len)
    ends = [sum(r[1] for r in runs[:i + 1]) for i in range(len(runs))]

    loads = [pltpu.make_async_copy(src, dst, load_sem.at[i]) for i, (src, dst) in enumerate(
        ((subject_hbm, subject_ref), (bold_hbm, bold_ref), (idx_hbm, idx_ref)))]
    for load in loads:
        load.start()
    greet_bx(count)
    loads[0].wait()
    named = jnp.broadcast_to(subject_ref[...], (epochs, LANES))
    named_t = named.T
    row = lax.broadcasted_iota(jnp.int32, (epochs, LANES), 0)
    col = lax.broadcasted_iota(jnp.int32, (epochs, LANES), 1)
    ahead = (named_t < named) | ((named_t == named) & (row < col))
    rank = jnp.sum(ahead.astype(jnp.float32), axis=0, keepdims=True).astype(jnp.int32)
    perm = (jnp.broadcast_to(rank, (epochs, LANES)) == row).astype(jnp.float32)
    perm_ref[...] = perm
    perm16 = perm.astype(jnp.bfloat16)

    loads[1].wait()

    def arrange(t, carry):
        sorted_ref[t] = jnp.dot(perm16, bold_ref[t], preferred_element_type=jnp.float32)
        return carry

    lax.fori_loop(0, points // 4, fourfold(arrange), 0)

    blank = jnp.zeros((LANES - depth, block_len), jnp.float32)

    def tile_of(i):
        return slice(i * LANES, (i + 1) * LANES)

    def join(low, high):
        return jnp.concatenate([low, high], axis=1)

    def turned(values):
        return join(values[:, HALF:], values[:, :HALF])

    def fill(g, carry):
        cells = normalized(sorted_ref[:, pl.ds(pl.multiple_of(g * GROUP, GROUP), GROUP), :])
        cells = cells.reshape(depth, block_len).astype(jnp.bfloat16)
        rows = pl.ds(pl.multiple_of(g * depth, depth), depth)
        here0, here1 = cells[:, :LANES], cells[:, LANES:]
        turn0, turn1 = turned(here0), turned(here1)
        win_ref[rows, tile_of(1)] = here0
        win_ref[rows, tile_of(2)] = here1
        win_ref[rows, tile_of(5)] = turn0
        win_ref[rows, tile_of(6)] = join(turn0[:, :HALF], turn1[:, HALF:])
        win_ref[rows, tile_of(7)] = turn1
        return carry

    lax.fori_loop(0, groups // 8, eightfold(fill), 0)

    def pair_rows(g):
        first = pl.multiple_of(g * depth, depth)
        return pl.ds(first, depth), pl.ds(pl.multiple_of(first + packed, depth), depth)

    def pack(quarters):
        def body(g, carry):
            upper, lower = pair_rows(g)
            for q in quarters:
                one, two = ((1, 5), (5, 1), (2, 7), (7, 2))[q]
                quarter_ref[q, upper, :] = join(
                    win_ref[upper, tile_of(one)][:, :HALF], win_ref[lower, tile_of(two)][:, HALF:])
            return carry

        lax.fori_loop(0, groups // 8, fourfold(body), 0)

    pack((0, 3))
    pl.semaphore_wait(pltpu.get_barrier_semaphore(), count - 1)

    def message(side, phase):
        quarter = (3 - phase) if side == 0 else phase
        to = me + 1 if side == 0 else me - 1
        return pltpu.make_async_remote_copy(
            src_ref=quarter_ref.at[quarter], dst_ref=halo_ref.at[side * 3 + phase],
            send_sem=send0.at[side * 3 + phase], recv_sem=recv0.at[side * 3 + phase],
            device_id={"bx": to}, device_id_type=MESH)

    sends = (me < count - 1, me > 0)
    gets = (me > 0, me < count - 1)
    def send(phase):
        for side in range(2):
            @pl.when(sends[side])
            def _():
                message(side, phase).start()

    send(NEAR)
    pack((1, 2))

    for side in range(2):
        @pl.when(jnp.logical_not(gets[side]))
        def _():
            for phase in range(3):
                halo_ref[side * 3 + phase] = jnp.zeros((packed, LANES), jnp.bfloat16)

    one_row = subject_ref[...]
    starts = [jnp.clip(jnp.sum((one_row < s).astype(jnp.float32)).astype(jnp.int32), 0, epochs)
              for s in range(SUBJ + 1)]
    sid = jnp.zeros((epochs, LANES), jnp.int32)
    for s in range(1, SUBJ):
        sid = sid + (row >= starts[s]).astype(jnp.int32)
    sid_ref[...] = sid

    def turn_own(g, carry):
        rows = pl.ds(pl.multiple_of(g * depth, depth), depth)
        own = win_ref[rows, LANES:LANES + block_len].astype(jnp.float32)
        flat = jnp.concatenate([own, blank], axis=0).T
        for b in range(block_len // ROWS):
            piece = flat[b * ROWS:(b + 1) * ROWS, :]
            own_ref[b, g] = jnp.concatenate([piece, piece], axis=0).astype(jnp.bfloat16)
        return carry

    lax.fori_loop(0, groups // 8, eightfold(turn_own), 0)

    loads[2].wait()
    for half in range(block_len // LANES):
        at = idx_ref[:, half * LANES:(half + 1) * LANES].T
        centre = lax.broadcasted_iota(jnp.int32, (LANES, slots), 0) + half * LANES
        column = pick(centre // ROWS, sorted((r[2] + r[1], r[3]) for r in runs))
        offset = at - block_len - column
        part = slice(half * LANES, (half + 1) * LANES)
        valid_ref[part, :] = (at >= 0).astype(jnp.float32)
        lane_ref[part, :] = jnp.where(at >= 0, offset & (LANES - 1), 0)
        tile_ref[part, :] = jnp.where(at >= 0, offset >> 7, 0)

    def arrived(phase):
        for side in range(2):
            @pl.when(gets[side])
            def _():
                message(side, phase).wait_recv()

    def settle(phase):
        arrived(phase)
        if phase != EDGE:
            send(phase + 1)
        left, right = halo_ref.at[phase], halo_ref.at[3 + phase]
        inner_left, inner_right = (halo_ref.at[phase - 1], halo_ref.at[2 + phase]) if phase else (None, None)

        def body(g, carry):
            upper, lower = pair_rows(g)
            near_l, near_r = left[upper, :], right[upper, :]
            if phase == NEAR:
                for rows, (l, r) in ((upper, (near_l, near_r[:, :HALF])), (lower, (near_l[:, HALF:], near_r[:, HALF:]))):
                    win_ref[rows, tile_of(5)] = join(l[:, :HALF], win_ref[rows, tile_of(5)][:, HALF:])
                    win_ref[rows, tile_of(7)] = join(win_ref[rows, tile_of(7)][:, :HALF], r)
            else:
                in_l, in_r = inner_left[upper, :], inner_right[upper, :]
                a, b = (0, 3) if phase == FAR else (4, 8)
                for rows, cut in ((upper, slice(0, HALF)), (lower, slice(HALF, LANES))):
                    win_ref[rows, tile_of(a)] = join(near_l[:, cut], in_l[:, cut])
                    win_ref[rows, tile_of(b)] = join(in_r[:, cut], near_r[:, cut])
            return carry

        lax.fori_loop(0, groups // 8, fourfold(body), 0)

    total_ref[...] = jnp.zeros_like(total_ref)
    masks = []
    for p in range(GROUP // 2):
        which = lax.broadcasted_iota(jnp.int32, (2 * ROWS, LANES), 0) // ROWS + 2 * p
        lane = lax.broadcasted_iota(jnp.int32, (2 * ROWS, LANES), 1) % GROUP
        masks.append((which == lane).astype(jnp.float32).astype(jnp.bfloat16))
    inverse = [1.0 / jnp.maximum((starts[s + 1] - starts[s]).astype(jnp.float32), 1.0) for s in range(SUBJ)]
    for sum_ref, sq_ref in ((sum0_ref, sq0_ref), (sum1_ref, sq1_ref)):
        sum_ref[0] = jnp.zeros((ROWS, LANES), jnp.float32)
        sq_ref[0] = jnp.zeros((ROWS, LANES), jnp.float32)

    def nth(n):
        n = jnp.asarray(n, jnp.int32)
        block = n + pick(n, [(end, r[2] - (end - r[1])) for end, r in zip(ends, runs)])
        lane = pick(n, [(end, r[4]) for end, r in zip(ends, runs)])
        return block, pl.multiple_of(lane, LANES)

    def product(at, g):
        b, start = at
        rhs = win_ref[g * depth:(g + 1) * depth, pl.ds(start, SPAN)]
        own = own_ref[b, g]
        lhs = jnp.concatenate([own * m for m in masks], axis=0)[:, :depth]
        return jnp.dot(lhs, rhs, preferred_element_type=jnp.float32)

    def correlate(at, refs, queue, after):
        b = at[0]
        x_ref, sum_ref, sq_ref = refs[:3]
        here = pl.ds(pl.multiple_of(b * ROWS, ROWS), ROWS)
        lane = lane_ref[here, :]
        tile = tile_ref[here, :]
        first = tile == 0
        second = tile == 1
        running = jnp.zeros((ROWS, LANES), jnp.float32)
        squares = jnp.zeros((ROWS, LANES), jnp.float32)
        for g in range(groups):
            prod = queue.pop(0)
            for e in range(GROUP):
                r = e * ROWS
                parts = [take(prod[r:r + ROWS, t * LANES:(t + 1) * LANES], lane, BY_LANE)
                         for t in range(SPAN // LANES)]
                x = jnp.where(first, parts[0], jnp.where(second, parts[1], parts[2]))
                i = g * GROUP + e
                x_ref[i * ROWS:(i + 1) * ROWS, :] = x
                running = running + x
                squares = squares + x * x
                sum_ref[i + 1] = running
                sq_ref[i + 1] = squares
            ahead = g + AHEAD
            if ahead < groups:
                queue.append(product(at, ahead))
            elif after is not None:
                queue.append(product(after, ahead - groups))
            yield

    def kernels(b, refs):
        x_ref, sum_ref, sq_ref, mean_ref, scale_ref = refs
        valid = valid_ref[pl.ds(pl.multiple_of(b * ROWS, ROWS), ROWS), :]
        for s in range(SUBJ):
            mean = (sum_ref[starts[s + 1]] - sum_ref[starts[s]]) * inverse[s]
            second = (sq_ref[starts[s + 1]] - sq_ref[starts[s]]) * inverse[s]
            var = jnp.maximum(second - mean * mean, 0.0)
            mean_ref[s * ROWS:(s + 1) * ROWS, :] = mean
            scale_ref[s * ROWS:(s + 1) * ROWS, :] = lax.rsqrt(var + VARIANCE_FLOOR) * valid
        acc = None
        for r in range(ROWS):
            mean = mean_ref[pl.ds(r, SUBJ, stride=ROWS), :]
            scale = scale_ref[pl.ds(r, SUBJ, stride=ROWS), :]
            pieces = []
            for q in range(epochs // 8):
                at = sid_ref[q * 8:(q + 1) * 8, :]
                x = x_ref[pl.ds(q * 8 * ROWS + r, 8, stride=ROWS), :]
                pieces.append((x - take(mean, at, BY_ROW)) * take(scale, at, BY_ROW))
            feat = jnp.concatenate(pieces, axis=0).astype(jnp.bfloat16)
            kern = lax.dot_general(feat, feat, (((1,), (1,)), ((), ())), preferred_element_type=jnp.float32)
            part = jnp.sum((kern * kern).reshape(epochs // 8, 8, epochs), axis=0)
            square_ref[pl.ds(pl.multiple_of((b * ROWS + r) * 8, 8), 8), :] = part
            acc = kern if acc is None else acc + kern
            yield
        total_ref[...] += acc

    even = (x0_ref, sum0_ref, sq0_ref, mean0_ref, scale0_ref)
    odd = (x1_ref, sum1_ref, sq1_ref, mean1_ref, scale1_ref)
    blocks = block_len // ROWS

    def together(first, second):
        pace = groups // ROWS
        for _ in range(ROWS):
            for _ in range(pace):
                next(first)
            next(second)
        for rest in (first, second):
            for _ in rest:
                pass

    def keep(queue):
        for i, prod in enumerate(queue):
            prod_ref[i] = prod

    settle(NEAR)
    queue = [product(nth(0), g) for g in range(AHEAD)]
    for _ in correlate(nth(0), even, queue, nth(1)):
        pass
    keep(queue)
    near = sum(r[1] for r in runs if r[0] == NEAR)
    outer = sum(r[1] for r in runs if r[0] == EDGE)

    def two_blocks(j, carry):
        n = 2 * j

        @pl.when(j == (near - 3) // 2 + 1)
        def _():
            settle(FAR)

        @pl.when(j == (blocks - outer - 3) // 2 + 1)
        def _():
            settle(EDGE)

        queue = [prod_ref[i] for i in range(AHEAD)]
        last = nth(n + 2)
        together(correlate(nth(n + 1), odd, queue, last), kernels(nth(n)[0], even))
        together(correlate(last, even, queue, nth(n + 3)), kernels(nth(n + 1)[0], odd))
        keep(queue)
        return carry

    lax.fori_loop(0, blocks // 2 - 1, two_blocks, 0)
    queue = [prod_ref[i] for i in range(AHEAD)]
    together(correlate(nth(blocks - 1), odd, queue, None), kernels(nth(blocks - 2)[0], even))
    for _ in kernels(nth(blocks - 1)[0], odd):
        pass

    exact = lax.Precision.HIGHEST
    half_way = jnp.dot(total_ref[...], perm_ref[...], precision=exact, preferred_element_type=jnp.float32)
    total_ref[...] = jnp.dot(perm_ref[...].T, half_way, precision=exact, preferred_element_type=jnp.float32)
    for phase in range(3):
        for side in range(2):
            @pl.when(sends[side])
            def _():
                message(side, phase).wait_send()

    def spreads():
        for half in range(block_len // LANES):
            sums = None
            for r in range(8):
                part = square_ref[pl.ds(half * LANES * 8 + r, LANES, stride=8), :]
                sums = part if sums is None else sums + part
            sums = jnp.sum(sums.T, axis=0, keepdims=True)
            out_ref[epochs + half:epochs + half + 1, :] = jnp.sqrt(sums * (1.0 / (epochs * NB * NB)))

    reduce_over_bx(count, 1.0 / (NB * block_len * count), spreads, total_ref, out_ref, took_ref, send1, recv1, send2, recv2)


def per_device(bold, nbr_table, subject):
    epochs, points, block_len = bold.shape
    slots = nbr_table.shape[0]
    count = lax.axis_size("bx")
    bold = bold.transpose(1, 0, 2)
    vmem = pl.BlockSpec(memory_space=pltpu.VMEM)
    groups = epochs // GROUP
    f32 = functools.partial(pltpu.VMEM, dtype=jnp.float32)
    packed = pl.pallas_call(
        functools.partial(features_kernel, count),
        in_specs=[pl.BlockSpec(memory_space=pl.ANY)] * 3,
        out_specs=vmem,
        out_shape=jax.ShapeDtypeStruct((epochs + ROWS, epochs), jnp.float32),
        scratch_shapes=[
            f32((points, epochs, block_len)),
            pltpu.VMEM((points * epochs, 9 * LANES), jnp.bfloat16),
            pltpu.VMEM((4, points * epochs // 2, LANES), jnp.bfloat16),
            pltpu.VMEM((6, points * epochs // 2, LANES), jnp.bfloat16),
            pltpu.VMEM((block_len // ROWS, groups, 2 * ROWS, LANES), jnp.bfloat16),
            pltpu.VMEM((block_len, slots), jnp.int32),
            pltpu.VMEM((block_len, slots), jnp.int32),
            f32((block_len, slots)),
            pltpu.VMEM((epochs, LANES), jnp.int32),
            f32((epochs, epochs)),
            *[f32((epochs * ROWS, LANES))] * 2,
            *[f32((epochs + 1, ROWS, LANES))] * 4,
            *[f32((SUBJ * ROWS, LANES))] * 4,
            f32((block_len * 8, epochs)),
            f32((epochs, epochs)),
            f32((AHEAD, GROUP * ROWS, SPAN)),
            pltpu.VMEM((points, epochs, block_len), jnp.bfloat16),
            pltpu.VMEM((slots, block_len), jnp.int32),
            pltpu.VMEM((1, epochs), jnp.int32),
            pltpu.SemaphoreType.DMA((3,)),
            f32((count, epochs // owners_of(count)[0], epochs)),
            *[pltpu.SemaphoreType.DMA((6,))] * 2,
            *[pltpu.SemaphoreType.DMA((count,))] * 4,
        ],
        compiler_params=pltpu.CompilerParams(collective_id=0, has_side_effects=True,
                                             vmem_limit_bytes=60 * 1024 * 1024),
        name="features",
    )(bold, nbr_table, subject[None, :])
    spread = packed[epochs:epochs + block_len // LANES].reshape(block_len)
    return spread, packed[:epochs]


def solution(mesh):
    return jax.shard_map(
        per_device,
        mesh=mesh,
        in_specs=(P("cohort", None, "bx"), P("cohort", "bx"), P("cohort")),
        out_specs=(P(("cohort", "bx")), P("cohort", None)),
        check_vma=False,
    )
```
